512 devices in a mesh: groups: 2 (over y), tp: 16 (over x, core), kv: 16 (over z).
Axes of the slice: x: 8, y: 2, z: 16, core: 2. Of those that a mesh axis runs over, the one named last changes fastest.
The devices are a block of a 8x8x16 slice.
Arguments:
- prompt_rows: bfloat16 [1024, 8192], P('groups', 'kv'), parts along dimension 0, may hold values from -400 to 400
- step_rows: bfloat16 [4, 8192], P('groups', 'kv'), parts along dimension 0, may hold values from -400 to 400
- norm_gain: bfloat16 [8192], P('kv'), may hold values from 0.5 to 1.5
- w_query: bfloat16 [8192, 8192], P('kv', 'tp'), may hold values from -0.0625 to 0.0625
- w_key: bfloat16 [8192, 1024], P('kv', 'tp'), may hold values from -0.125 to 0.125
- w_value: bfloat16 [8192, 1024], P('kv', 'tp'), may hold values from -0.0625 to 0.0625
- w_output: bfloat16 [8192, 8192], P('tp', 'kv'), may hold values from -0.0625 to 0.0625
- kv_cache: bfloat16 [8, 16384, 4096], P('groups', 'kv', 'tp'), parts along dimension 0, may hold values from -250 to 250, as said below
- step_lengths: int32 [4], P('groups'), parts along dimension 0, may hold values from 4096 to 16383
- rollout_ids: int32 [4], P('groups'), parts along dimension 0, may hold values from 0 to 1, each once
- resume_offsets: int32 [4], P('groups'), parts along dimension 0, may hold values from 2048 to 15872
- stretch_rollout: int32 [1024], P('groups'), parts along dimension 0, may hold values from 0 to 1, never falling along the last dimension, each value on 1 to 384 neighbouring positions
Outputs:
- prompt_out: bfloat16 [1024, 8192], P(('groups', 'tp'), 'kv'), parts along dimension 0
- step_out: bfloat16 [4, 8192], P('groups', 'kv'), parts along dimension 0
The draws below stay inside these ranges and needn't reach their ends.
There are 2 independent parts, one for each index of `groups`. The reference program is written for one: setup_inputs(seed, part) draws one part's arguments, and reference() takes and returns one part's arrays. A program takes and returns all parts, laid end to end along the dimension named above; an argument that names none is the same for every part. Nothing has to cross between parts.
Inputs may be any that keep to these rules, and one draw needn't show every extreme that they name: `kv_cache`: along the last dimension, block t of 16 holds for each j below 1 the keys then the values (128 entries each) of key-value head (t * 4) // 8 + j; blocks naming the same head are equal.
All inputs are finite; a program needn't handle non-finite values.
Results may differ from the reference program's by a relative error of at most 0.012.
The reference program's roundings to bfloat16 on the way count: a program that leaves them out, or rounds other values in their place, can miss the bound.
Values may be sent and summed in bfloat16 or wider, within the bound.
No kernel may reach another device: no remote copies, remote signals or barrier semaphores. Data moves between devices by JAX's collectives and lax.ppermute only.
A program may use at most 64 MiB of HBM per device.

```python
import math
import jax
import jax.numpy as jnp
import numpy as np
from jax import lax

D = 8192
H = 64
KVH = 8
HD = 128
STRETCH = 512
SEQS = 2
ROLL = 2
LMAX = 16384
QPK = 8
HQL = 4
KV_DEV = 1
SLOTS = 4
SEG_MOST = 384
N_TP = 16


def activation(key, row_count):
    key_base = jax.random.fold_in(key, 0)
    column = jnp.exp(jnp.arange(D, dtype=jnp.float32) * (math.log(3.0) / D))
    base_draw = jnp.clip(jax.random.normal(key_base, (row_count, D), jnp.float32), -5.0, 5.0)
    result = base_draw * column[None, :]
    return result.astype(jnp.bfloat16)


def draw_prompt_rows(key, part):
    return activation(jax.random.fold_in(key, 11), STRETCH)


def draw_step_rows(key, part):
    return activation(jax.random.fold_in(key, 13), SEQS)


def draw_kv_cache(key, part):
    key_base = jax.random.fold_in(jax.random.fold_in(key, 17), 0)
    full_shape = (SLOTS, LMAX, KVH, 2, HD)
    kind_scale = jnp.array([2.0, 1.0], jnp.float32)[None, None, None, :, None]
    canon = jnp.clip(jax.random.normal(key_base, full_shape, jnp.float32), -4.0, 4.0) * kind_scale
    head_table = np.array([tp_rank * HQL // QPK + local for tp_rank in range(N_TP) for local in range(KV_DEV)], dtype=np.int32)
    copied = canon[:, :, head_table]
    return copied.reshape(SLOTS, LMAX, N_TP * KV_DEV * 2 * HD).astype(jnp.bfloat16)


def levels(own_key, dims, shards, least, high):
    gain, own = 1.0, jax.random.fold_in(own_key, 6)
    for dim, parts in shards:
        heights = jnp.exp(jax.random.uniform(jax.random.fold_in(own, dim), (parts,), jnp.float32, least / len(shards), high / len(shards)))
        gain = gain * jnp.repeat(heights, dims[dim] // parts).reshape([-1 if axis == dim else 1 for axis in range(len(dims))])
    return gain


def split_up(count, total, limit, skew):
    weights = [(1 << 20) // math.isqrt(standing ** skew) + 1 for standing in range(2, count + 1)]
    rest, given = total - limit - (count - 1), [1] * (count - 1)
    while rest > 0:
        movable = [i for i in range(count - 1) if given[i] < limit]
        whole, budget = sum([weights[i] for i in movable]), rest
        for i in movable:
            extra = min(limit - given[i], max(1, budget * weights[i] // whole), rest)
            given[i] = given[i] + extra
            rest = rest - extra
    return np.array([limit] + given)


def uneven(key, count, total, limit, slope):
    if count == 2:
        one = jax.random.randint(key, (), max(1, total - limit), min(limit, total - 1) + 1)
        return jnp.stack([one, total - one])
    tallies = jnp.asarray(split_up(count, total, limit, slope), jnp.int32)
    pairs = (count - 1) // 2
    source_of, taker = tallies[1:1 + 2 * pairs:2], tallies[2:2 + 2 * pairs:2]
    room = jnp.minimum(source_of - 1, limit - taker)
    moved = jax.random.randint(jax.random.fold_in(key, 1), (pairs,), 0, 1 << 20) % (room + 1)
    tallies = tallies.at[1:1 + 2 * pairs:2].set(source_of - moved).at[2:2 + 2 * pairs:2].set(taker + moved)
    return tallies[jax.random.permutation(jax.random.fold_in(key, 2), count)]


def bell_draw(rng, extent, width, bound, shards=(), kind=jnp.bfloat16):
    drawn = width * jax.random.normal(rng, extent, jnp.float32)
    if shards:
        drawn = drawn * levels(rng, extent, shards, -0.22, 0.18)
    return jnp.clip(drawn, -bound, bound).astype(kind)


def setup_inputs(seed: int = 0, part: int = 0) -> dict:
    splits = jax.random.split(jax.random.key(seed), 13)
    part_splits = jax.random.split(jax.random.fold_in(splits[12], part), 13)
    return {
        "prompt_rows": draw_prompt_rows(jax.random.fold_in(jax.random.fold_in(splits[12], part), 71), part),
        "step_rows": draw_step_rows(jax.random.fold_in(jax.random.fold_in(splits[12], part), 71), part),
        "norm_gain": jnp.clip(1.0 + 0.1 * jax.random.normal(splits[2], (D,), jnp.float32), 0.5, 1.5).astype(jnp.bfloat16),
        "w_query": bell_draw(splits[3], (D, H * HD), D ** -0.5, 0.0625, ((0, 16), (1, 16))),
        "w_key": bell_draw(splits[4], (D, KVH * HD), (D // 4) ** -0.5, 0.125, ((0, 16), (1, 16))),
        "w_value": bell_draw(splits[5], (D, KVH * HD), D ** -0.5, 0.0625, ((0, 16), (1, 16))),
        "w_output": bell_draw(splits[6], (H * HD, D), (H * HD) ** -0.5, 0.0625, ((0, 16), (1, 16))),
        "kv_cache": draw_kv_cache(jax.random.fold_in(jax.random.fold_in(splits[12], part), 71), part),
        "step_lengths": jax.random.randint(part_splits[8], (SEQS,), LMAX // 4, LMAX).astype(jnp.int32),
        "rollout_ids": jax.random.permutation(part_splits[9], ROLL).astype(jnp.int32),
        "resume_offsets": jax.random.randint(part_splits[10], (ROLL,), LMAX // 8, LMAX - STRETCH + 1).astype(jnp.int32),
        "stretch_rollout": jnp.searchsorted(jnp.cumsum(uneven(part_splits[11], ROLL, STRETCH, SEG_MOST, 0)), jnp.arange(STRETCH), side="right").astype(jnp.int32),
    }


EPSILON = 1e-05
THETA = 500000.0
NEGATIVE = -1e+30

def rotate(values, positions):
    half_dim = values.shape[-1] // 2
    freq_index = jnp.arange(half_dim, dtype=jnp.float32)
    inverse = jnp.exp(freq_index * (-2.0 * math.log(THETA) / values.shape[-1]))
    angles = positions.astype(jnp.float32)[:, None] * inverse[None, :]
    cosine = jnp.cos(angles)[:, None, :]
    sine_part = jnp.sin(angles)[:, None, :]
    first_half = values[..., :half_dim]
    second_half = values[..., half_dim:]
    return jnp.concatenate([first_half * cosine - second_half * sine_part, second_half * cosine + first_half * sine_part], axis=-1)

def stretch_positions(stretch_rollout, resume_offsets):
    members = jnp.arange(resume_offsets.shape[0], dtype=jnp.int32)
    onehot = (stretch_rollout[:, None] == members[None, :]).astype(jnp.int32)
    starts = lax.optimization_barrier(jnp.sum((stretch_rollout[:, None] < members[None, :]).astype(jnp.int32), axis=0))
    shifted = lax.optimization_barrier(jnp.sum(onehot * (resume_offsets - starts)[None, :], axis=1))
    return shifted + jnp.arange(stretch_rollout.shape[0], dtype=jnp.int32)

def normalized_mix(scores, allowed, values, form):
    masked = jnp.where(allowed, scores, NEGATIVE)
    top_score = lax.optimization_barrier(jnp.max(masked, axis=-1, keepdims=True))
    weights = jnp.where(allowed, jnp.exp(scores - top_score), 0.0)
    denominator = lax.optimization_barrier(jnp.sum(weights, axis=-1))
    rounded = lax.optimization_barrier(weights.astype(jnp.bfloat16)).astype(jnp.float32)
    mixed_out = jnp.einsum(form, rounded, values.astype(jnp.float32))
    return (mixed_out / denominator[..., None]).astype(jnp.bfloat16)

def reference(prompt_rows, step_rows, norm_gain, w_query, w_key, w_value, w_output, kv_cache, step_lengths, rollout_ids, resume_offsets, stretch_rollout):
    all_rows = jnp.concatenate([prompt_rows, step_rows], axis=0)
    widened = all_rows.astype(jnp.float32)
    norm_scale = lax.rsqrt(lax.optimization_barrier(jnp.sum(widened * widened, axis=1)) / D + EPSILON)
    normed = (widened * norm_gain.astype(jnp.float32)[None, :]).astype(jnp.bfloat16)
    row_count = all_rows.shape[0]
    query_raw = jnp.dot(normed, w_query, preferred_element_type=jnp.float32) * norm_scale[:, None]
    key_raw = jnp.dot(normed, w_key, preferred_element_type=jnp.float32) * norm_scale[:, None]
    value_rows = (jnp.dot(normed, w_value, preferred_element_type=jnp.float32) * norm_scale[:, None]).astype(jnp.bfloat16)
    value_rows = lax.optimization_barrier(value_rows).reshape(row_count, KVH, HD)
    positions = jnp.concatenate([stretch_positions(stretch_rollout, resume_offsets), step_lengths.astype(jnp.int32)])
    query_rows = lax.optimization_barrier(rotate(query_raw.reshape(row_count, H, HD), positions).astype(jnp.bfloat16))
    key_rows = lax.optimization_barrier(rotate(key_raw.reshape(row_count, KVH, HD), positions).astype(jnp.bfloat16))
    layout = kv_cache.reshape(SLOTS, LMAX, N_TP, KV_DEV, 2, HD)
    owners = np.array([kv_head * QPK // HQL for kv_head in range(KVH)], dtype=np.int32)
    within = np.array([kv_head - kv_head * QPK // HQL * HQL // QPK for kv_head in range(KVH)], dtype=np.int32)
    canon = layout[:, :, owners, within]
    rollout_cache = canon[SEQS + rollout_ids.astype(jnp.int32)]
    step_cache = canon[:SEQS]
    members = jnp.arange(ROLL, dtype=jnp.int32)
    key_index = jnp.arange(LMAX, dtype=jnp.int32)
    in_member = stretch_rollout[:, None] == members[None, :]
    before = key_index[None, :] < resume_offsets[:, None]
    cache_mask = (in_member[:, :, None] & before[None, :, :]).reshape(STRETCH, ROLL * LMAX)
    stretch_index = jnp.arange(STRETCH, dtype=jnp.int32)
    stretch_mask = (stretch_rollout[:, None] == stretch_rollout[None, :]) & (stretch_index[None, :] <= stretch_index[:, None])
    prompt_mask = jnp.concatenate([cache_mask, stretch_mask], axis=1)[:, None, :]
    step_mask = jnp.concatenate([key_index[None, :] < step_lengths[:, None], jnp.ones((SEQS, 1), dtype=bool)], axis=1)[:, None, :]
    inverse_root = 1.0 / math.sqrt(HD)

    def one_head(kv_head):
        group_query = lax.dynamic_slice_in_dim(query_rows, kv_head * QPK, QPK, 1).astype(jnp.float32)
        own_keys = lax.dynamic_index_in_dim(key_rows, kv_head, 1, keepdims=False)
        own_values = lax.dynamic_index_in_dim(value_rows, kv_head, 1, keepdims=False)
        head_cache = lax.dynamic_index_in_dim(rollout_cache, kv_head, 2, keepdims=False)
        prompt_keys = jnp.concatenate([head_cache[:, :, 0].reshape(ROLL * LMAX, HD), own_keys[:STRETCH]], axis=0)
        prompt_values = jnp.concatenate([head_cache[:, :, 1].reshape(ROLL * LMAX, HD), own_values[:STRETCH]], axis=0)
        prompt_scores = jnp.einsum('qgd,kd->qgk', group_query[:STRETCH], prompt_keys.astype(jnp.float32)) * inverse_root
        prompt_mix = normalized_mix(prompt_scores, prompt_mask, prompt_values, 'qgk,kd->qgd')
        step_head = lax.dynamic_index_in_dim(step_cache, kv_head, 2, keepdims=False)
        step_keys = jnp.concatenate([step_head[:, :, 0], own_keys[STRETCH:][:, None, :]], axis=1)
        step_values = jnp.concatenate([step_head[:, :, 1], own_values[STRETCH:][:, None, :]], axis=1)
        step_scores = jnp.einsum('sgd,skd->sgk', group_query[STRETCH:], step_keys.astype(jnp.float32)) * inverse_root
        step_mix = normalized_mix(step_scores, step_mask, step_values, 'sgk,skd->sgd')
        return (prompt_mix, step_mix)
    prompt_mix, step_mix = lax.map(one_head, jnp.arange(KVH, dtype=jnp.int32))
    prompt_mix = jnp.transpose(prompt_mix, (1, 0, 2, 3)).reshape(STRETCH, H * HD)
    step_mix = jnp.transpose(step_mix, (1, 0, 2, 3)).reshape(SEQS, H * HD)
    prompt_out = jnp.dot(prompt_mix, w_output, preferred_element_type=jnp.float32).astype(jnp.bfloat16)
    step_out = jnp.dot(step_mix, w_output, preferred_element_type=jnp.float32).astype(jnp.bfloat16)
    return (prompt_out, step_out)
```

```python
import functools
import math

import jax
import jax.numpy as jnp
from jax import lax
from jax.experimental import pallas as pl
from jax.experimental.pallas import tpu as pltpu
from jax.sharding import PartitionSpec as P

HD = 128
SEQS = 2
EPSILON = 1e-05
THETA = 500000.0
NEGATIVE = -1e30
TAIL = 8
F32 = jnp.float32
BF16 = jnp.bfloat16
VMEM = pltpu.VMEM
SMEM = pltpu.SMEM


def call(body, outs, spaces, flops, traffic, scratch=(), name=None):
    return pl.pallas_call(
        body,
        out_shape=outs,
        in_specs=[pl.BlockSpec(memory_space=s) for s in spaces],
        out_specs=jax.tree.map(lambda _: pl.BlockSpec(memory_space=VMEM), outs),
        scratch_shapes=list(scratch),
        compiler_params=pltpu.CompilerParams(vmem_limit_bytes=48 * 1024 * 1024),
        cost_estimate=pl.CostEstimate(flops=flops, bytes_accessed=traffic, transcendentals=0),
        name=name,
    )


def two_terms(value):
    high = value.astype(BF16).astype(F32)
    return high, value - high


def three_terms(value):
    high, rest = two_terms(value)
    mid, low = two_terms(rest)
    return high, mid, low


def stacked_rows(rows):
    place = lax.broadcasted_iota(jnp.int32, (TAIL, HD), 0)
    block = jnp.zeros((TAIL, HD), F32)
    for k, row in enumerate(rows):
        block = jnp.where(place == k, jnp.broadcast_to(row, (TAIL, HD)), block)
    return block


def turned(values, cosines, sines):
    half = HD // 2
    swapped = jnp.concatenate([values[:, half:], values[:, :half]], axis=1)
    return values * cosines + swapped * sines


def project(prompt, step, gain, w_query, w_key, w_value, out, step_pad):
    count, share = out.shape[0], prompt.shape[0] // out.shape[0]
    heads = w_query.shape[1] // HD
    steps = step.shape[0]
    wide = prompt[...].astype(F32)
    scale = gain[...].astype(F32)
    normed = (wide * scale).astype(BF16)
    step_pad[...] = jnp.zeros_like(step_pad)
    step_pad[0:steps, :] = step[...].astype(F32)
    step_wide = step_pad[...]
    step_normed = (step_wide * scale).astype(BF16)
    pair_weight = jnp.concatenate([w_key[...], w_value[...]], axis=1)
    step_pieces = []
    for c in range(0, heads, 2):
        weight = w_query[:, c * HD : (c + 2) * HD]
        part = jnp.dot(normed, weight, preferred_element_type=F32).astype(BF16)
        for k in range(2):
            out[:, (c + k) * share : (c + k + 1) * share, :] = part[
                :, k * HD : (k + 1) * HD
            ].reshape(count, share, HD)
        small = jnp.dot(step_normed, weight, preferred_element_type=F32)
        step_pieces += [small[:, :HD], small[:, HD:]]
    part = jnp.dot(normed, pair_weight, preferred_element_type=F32).astype(BF16)
    out[:, heads * share : (heads + 1) * share, :] = part.reshape(count, share, HD)
    step_pieces.append(jnp.dot(step_normed, pair_weight, preferred_element_type=F32))
    square = wide * wide
    high, low = two_terms(square)
    ones = jnp.ones((TAIL, prompt.shape[1]), BF16)
    dims = (((1,), (1,)), ((), ()))
    sums = lax.dot_general(ones, high.astype(BF16), dims, preferred_element_type=F32)
    sums = sums + lax.dot_general(ones, low.astype(BF16), dims, preferred_element_type=F32)
    sums = sums[0:1, :]
    step_sums = jnp.sum(step_wide * step_wide, axis=1, keepdims=True)
    for d in range(count):
        lane = d * share // HD * HD
        rows = list(two_terms(sums[:, lane : lane + HD]))
        s, c = divmod(d, heads + 1)
        if s < steps:
            rows = [step_pieces[c][s : s + 1, :], *rows]
            rows += [jnp.broadcast_to(t, (1, HD)) for t in two_terms(step_sums[s : s + 1, :])]
        else:
            rows = [jnp.zeros((1, HD), F32), *rows]
        out[d, (heads + 1) * share : (heads + 1) * share + TAIL, :] = stacked_rows(rows).astype(
            BF16
        )


def complete(where, tiles, cosines, sines, query_out, pair_out, *, features):
    count = tiles.shape[0]
    share = cosines.shape[0] - TAIL
    heads = (query_out.shape[0] - TAIL) // share

    def total(start, size):
        return jnp.sum(tiles[:, start : start + size, :].astype(F32), axis=0)

    tail = total((heads + 1) * share, TAIL)
    row_scale = lax.rsqrt((tail[1:2, :] + tail[2:3, :]) / features + EPSILON)
    offset = lax.rem(where[0] * share, HD)
    place = lax.broadcasted_iota(jnp.int32, (share, HD), 0) + offset
    lane = lax.broadcasted_iota(jnp.int32, (share, HD), 1)
    scale = jnp.sum(
        jnp.where(place == lane, jnp.broadcast_to(row_scale, (share, HD)), 0.0),
        axis=1,
        keepdims=True,
    )
    step_scale = lax.rsqrt((tail[3:4, :] + tail[4:5, :]) / features + EPSILON)
    first = lax.broadcasted_iota(jnp.int32, (TAIL, HD), 0) == 0
    step_value = jnp.where(first, jnp.broadcast_to(tail[0:1, :] * step_scale, (TAIL, HD)), 0.0)
    cosine, sine = cosines[0:share, :], sines[0:share, :]
    for c in range(heads):
        value = total(c * share, share) * scale
        query_out[c * share : (c + 1) * share, :] = turned(value, cosine, sine).astype(BF16)
    query_out[heads * share : heads * share + TAIL, :] = turned(
        step_value, cosines[share:, :], sines[share:, :]
    ).astype(BF16)
    pair_out[0:share, :] = total(heads * share, share) * scale
    pair_out[share : share + TAIL, :] = step_value


def attend(
    where,
    starts,
    slots,
    offsets,
    lengths,
    queries,
    own_pair,
    other_pair,
    cosines,
    sines,
    cache,
    out,
    own_keys,
    own_values,
    step_query,
    *,
    steps,
    group,
):
    count = queries.shape[0]
    share = cosines.shape[0] - TAIL
    heads = (queries.shape[1] - TAIL) // share
    rows = heads * share
    block = cache.shape[1]
    members = slots.shape[0]
    half = HD // 2
    mine = where[0]
    first = where[1] == 0
    root = 1.0 / math.sqrt(HD)
    low_half = jnp.where(first, own_pair[...], other_pair[...])
    high_half = jnp.where(first, other_pair[...], own_pair[...])
    raw_keys = jnp.concatenate([low_half[:, :half], high_half[:, :half]], axis=1)
    raw_values = jnp.concatenate([low_half[:, half:], high_half[:, half:]], axis=1)
    own_keys[...] = jnp.zeros_like(own_keys)
    own_values[...] = jnp.zeros_like(own_values)
    turned_keys = turned(raw_keys, cosines[...], sines[...])
    own_keys[0 : share + TAIL, :] = turned_keys
    own_values[0 : share + TAIL, :] = raw_values
    keys_here = own_keys[...].astype(BF16)
    values_here = own_values[...].astype(BF16)
    dims = (((1,), (1,)), ((), ()))
    key_place = lax.broadcasted_iota(jnp.int32, (1, block), 1) + mine * block
    tile = group * rows
    place = lax.broadcasted_iota(jnp.int32, (tile, HD), 0)
    token_in_tile = place // rows * share + lax.rem(place, share)
    lane = lax.broadcasted_iota(jnp.int32, (tile, HD), 1)
    key_token = mine * share + lane
    square_row = lax.broadcasted_iota(jnp.int32, (rows, HD), 0)
    square_lane = lax.broadcasted_iota(jnp.int32, (rows, HD), 1)

    step_rows = {}
    for s in range(steps):
        step_query[...] = jnp.zeros_like(step_query)
        for h in range(heads):
            step_query[h : h + 1, :] = queries[s * (heads + 1) + h, rows : rows + TAIL, :].astype(
                F32
            )[0:1, :]
        query = step_query[...]
        bias = jnp.where(key_place < lengths[s], 0.0, NEGATIVE)
        scores = (
            lax.dot_general(
                query.astype(BF16), cache[s, :, 0:HD], dims, preferred_element_type=F32
            )
            * root
            + bias
        )
        own_key = own_keys[share : share + 1, :].astype(BF16).astype(F32)
        own_value = own_values[share : share + 1, :].astype(BF16).astype(F32)
        own = jnp.sum(query * own_key, axis=1, keepdims=True) * root
        own = jnp.where(mine == s * (heads + 1) + heads, own, NEGATIVE)
        top = jnp.maximum(jnp.max(scores, axis=1, keepdims=True), own)
        weights = jnp.exp(scores - top)
        own_weight = jnp.exp(own - top)
        denominator = jnp.sum(weights, axis=1, keepdims=True) + own_weight
        mixed = jnp.dot(weights.astype(BF16), cache[s, :, HD:], preferred_element_type=F32)
        mixed = mixed + own_weight.astype(BF16).astype(F32) * own_value
        mixed = mixed / denominator
        level = top + jnp.log(denominator)
        for h in range(heads):
            step_rows[s * heads + h] = [mixed[h : h + 1, :]] + [
                jnp.broadcast_to(t, (1, HD)) for t in three_terms(level[h : h + 1, :])
            ]

    for t in range(count // group):
        begin = t * group * share
        token = token_in_tile + begin
        query = queries[t * group : (t + 1) * group, 0:rows, :].reshape(tile, HD)
        scored = lax.dot_general(query, keys_here, dims, preferred_element_type=F32) * root

        for r in range(members):
            since = starts[r]
            until = starts[r + 1]

            @pl.when((since < begin + group * share) & (until > begin))
            def _():
                inside = (key_token >= since) & (key_token <= token) & (lane < share)
                own = jnp.where(inside, scored, NEGATIVE)
                slot = SEQS + slots[r]
                bias = jnp.where(key_place < offsets[r], 0.0, NEGATIVE)
                scores = (
                    lax.dot_general(
                        query, cache[slot, :, 0:HD], dims, preferred_element_type=F32
                    )
                    * root
                    + bias
                )
                top = jnp.maximum(
                    jnp.max(scores, axis=1, keepdims=True), jnp.max(own, axis=1, keepdims=True)
                )
                weights = jnp.exp(scores - top)
                own_weights = jnp.exp(own - top)
                denominator = jnp.sum(weights, axis=1, keepdims=True) + jnp.sum(
                    own_weights, axis=1, keepdims=True
                )
                mixed = jnp.dot(
                    weights.astype(BF16), cache[slot, :, HD:], preferred_element_type=F32
                )
                mixed = mixed + jnp.dot(
                    own_weights.astype(BF16), values_here, preferred_element_type=F32
                )
                mixed = (mixed / denominator).astype(BF16)
                level = top + jnp.log(denominator)
                for g in range(group):
                    d = t * group + g
                    piece = mixed[g * rows : (g + 1) * rows, :]
                    flat = jnp.sum(
                        jnp.where(
                            square_row == square_lane,
                            jnp.broadcast_to(level[g * rows : (g + 1) * rows, :], (rows, HD)),
                            0.0,
                        ),
                        axis=0,
                        keepdims=True,
                    )
                    full = list(three_terms(flat)) + step_rows.get(d, [])
                    tail = stacked_rows(full).astype(BF16)

                    @pl.when(since <= begin + g * share)
                    def _():
                        out[d, 0:rows, :] = piece
                        out[d, rows : rows + TAIL, :] = tail

                    @pl.when(since > begin + g * share)
                    def _():
                        late = (
                            lax.rem(square_row, share) + (begin + g * share) >= since
                        )
                        before = out[d, 0:rows, :].astype(F32)
                        out[d, 0:rows, :] = jnp.where(late, piece.astype(F32), before).astype(BF16)
                        late_lane = (
                            lax.rem(square_lane, share) + (begin + g * share) >= since
                        )[0:TAIL, :]
                        stays = lax.broadcasted_iota(jnp.int32, (TAIL, HD), 0) >= 3
                        earlier = out[d, rows : rows + TAIL, :].astype(F32)
                        out[d, rows : rows + TAIL, :] = jnp.where(
                            late_lane | stays, tail.astype(F32), earlier
                        ).astype(BF16)


def combine(tiles, out, levels):
    count = tiles.shape[0]
    rows = tiles.shape[1] - TAIL
    tail = tiles[:, rows : rows + TAIL, :].astype(F32)
    level = tail[:, 0, :] + tail[:, 1, :] + tail[:, 2, :]
    weight = jnp.exp(level - jnp.max(level, axis=0, keepdims=True))
    weight = weight / jnp.sum(weight, axis=0, keepdims=True)
    levels[...] = jnp.zeros_like(levels)
    levels[0:count, :] = weight
    across = jnp.transpose(levels[...])
    mixed = jnp.zeros((rows, HD), F32)
    for k in range(count):
        mixed = mixed + across[:, k : k + 1] * tiles[k, 0:rows, :].astype(F32)
    out[0:rows, :] = mixed.astype(BF16)
    level = tail[:, 4, :] + tail[:, 5, :] + tail[:, 6, :]
    weight = jnp.exp(level - jnp.max(level, axis=0, keepdims=True))
    weight = weight / jnp.sum(weight, axis=0, keepdims=True)
    step = jnp.sum(weight * tail[:, 3, :], axis=0, keepdims=True)
    out[rows : rows + TAIL, :] = jnp.broadcast_to(step, (TAIL, HD)).astype(BF16)


def deliver(mix, w_output, out, step_pad, *, steps):
    count = mix.shape[0]
    heads = w_output.shape[0] // HD
    share = (mix.shape[1] - TAIL) // heads
    takers = out.shape[0]
    wide = w_output.shape[1] // HD
    taken = count * share // takers
    block = jnp.concatenate(
        [
            mix[:, h * share : (h + 1) * share, :].reshape(count * share, HD)
            for h in range(heads)
        ],
        axis=1,
    )
    step_pad[...] = jnp.zeros_like(step_pad)
    for s in range(steps):
        for h in range(heads):
            step_pad[s : s + 1, h * HD : (h + 1) * HD] = mix[
                s * heads + h, heads * share : heads * share + TAIL, :
            ].astype(F32)[0:1, :]
    small = jnp.dot(step_pad[...].astype(BF16), w_output[...], preferred_element_type=F32)
    tail = stacked_rows(
        [small[s : s + 1, c * HD : (c + 1) * HD] for s in range(steps) for c in range(wide)]
    ).astype(BF16)
    for c in range(0, wide, 2):
        part = jnp.dot(
            block, w_output[:, c * HD : (c + 2) * HD], preferred_element_type=F32
        ).astype(BF16)
        for k in range(2):
            out[:, (c + k) * taken : (c + k + 1) * taken, :] = part[
                :, k * HD : (k + 1) * HD
            ].reshape(takers, taken, HD)
    for d in range(takers):
        out[d, wide * taken : wide * taken + TAIL, :] = tail


def settle(tiles, prompt_out, step_out):
    taken, width = prompt_out.shape
    wide = width // HD
    for c in range(wide):
        prompt_out[:, c * HD : (c + 1) * HD] = jnp.sum(
            tiles[:, c * taken : (c + 1) * taken, :].astype(F32), axis=0
        ).astype(BF16)
    tail = jnp.sum(tiles[:, wide * taken : wide * taken + TAIL, :].astype(F32), axis=0)
    for s in range(step_out.shape[0]):
        for c in range(wide):
            step_out[s : s + 1, c * HD : (c + 1) * HD] = tail[
                s * wide + c : s * wide + c + 1, :
            ].astype(BF16)


def on_device(
    prompt_rows,
    step_rows,
    norm_gain,
    w_query,
    w_key,
    w_value,
    w_output,
    kv_cache,
    step_lengths,
    rollout_ids,
    resume_offsets,
    stretch_rollout,
):
    kv_index = lax.axis_index("kv")
    kv_count = lax.axis_size("kv")
    tp_index = lax.axis_index("tp")
    tp_count = lax.axis_size("tp")
    tokens, width = prompt_rows.shape
    steps = step_rows.shape[0]
    heads = w_query.shape[1] // HD
    share = tokens // kv_count
    taken = tokens // tp_count
    rows = heads * share
    members = resume_offsets.shape[0]
    where = jnp.stack([kv_index, lax.rem(tp_index, 2)]).astype(jnp.int32)

    parts = call(
        project,
        jax.ShapeDtypeStruct((kv_count, rows + share + TAIL, HD), BF16),
        [VMEM] * 6,
        2 * tokens * width * (w_query.shape[1] + HD),
        4 * tokens * width,
        [pltpu.VMEM((16, width), F32)],
        "project",
    )(prompt_rows, step_rows, norm_gain.reshape(1, width), w_query, w_key, w_value)
    parts = lax.all_to_all(parts, "kv", 0, 0, tiled=True)

    member_index = jnp.arange(members + 1, dtype=jnp.int32)
    starts = jnp.sum(
        (stretch_rollout[:, None] < member_index[None, :]).astype(jnp.int32), axis=0
    )
    tokens_here = kv_index * share + jnp.arange(share, dtype=jnp.int32)
    rollout_here = jnp.sum(
        (tokens_here[:, None] >= starts[None, 1:members]).astype(jnp.int32), axis=1
    )
    onehot = (rollout_here[:, None] == member_index[None, :members]).astype(jnp.int32)
    positions = jnp.sum(onehot * (resume_offsets - starts[:members])[None, :], axis=1) + tokens_here
    step_place = jnp.minimum(kv_index // (heads + 1), steps - 1)
    step_position = lax.dynamic_slice_in_dim(step_lengths, step_place, 1, 0)
    positions = jnp.concatenate([positions, jnp.broadcast_to(step_position, (TAIL,))])
    half = HD // 2
    inverse = jnp.exp(jnp.arange(half, dtype=F32) * (-2.0 * math.log(THETA) / HD))
    angles = positions.astype(F32)[:, None] * inverse[None, :]
    cosine, sine = jnp.cos(angles), jnp.sin(angles)
    cosines = jnp.concatenate([cosine, cosine], axis=1)
    sines = jnp.concatenate([-sine, sine], axis=1)

    query_here, pair_here = call(
        functools.partial(complete, features=width * kv_count),
        (
            jax.ShapeDtypeStruct((rows + TAIL, HD), BF16),
            jax.ShapeDtypeStruct((share + TAIL, HD), F32),
        ),
        [SMEM] + [VMEM] * 3,
        2 * kv_count * rows * HD,
        2 * kv_count * rows * HD,
        name="complete",
    )(where, parts, cosines, sines)
    pair_there = lax.ppermute(pair_here, "tp", [(k, k ^ 1) for k in range(tp_count)])
    queries = lax.all_gather(query_here, "kv", axis=0)

    group = 4
    mixed = call(
        functools.partial(attend, steps=steps, group=group),
        jax.ShapeDtypeStruct((kv_count, rows + TAIL, HD), BF16),
        [SMEM] * 5 + [VMEM] * 6,
        4 * tokens * heads * kv_cache.shape[1] * HD,
        2 * kv_cache.size,
        [
            pltpu.VMEM((HD, HD), F32),
            pltpu.VMEM((HD, HD), F32),
            pltpu.VMEM((16, HD), F32),
        ],
        "attend",
    )(
        where,
        starts,
        rollout_ids,
        resume_offsets,
        step_lengths,
        queries,
        pair_here,
        pair_there,
        cosines,
        sines,
        kv_cache,
    )
    mixed = lax.all_to_all(mixed, "kv", 0, 0, tiled=True)
    mix_here = call(
        combine,
        jax.ShapeDtypeStruct((rows + TAIL, HD), BF16),
        [VMEM],
        2 * kv_count * rows * HD,
        2 * kv_count * rows * HD,
        [pltpu.VMEM((HD, HD), F32)],
        "combine",
    )(mixed)
    mix = lax.all_gather(mix_here, "kv", axis=0)
    shares = call(
        functools.partial(deliver, steps=steps),
        jax.ShapeDtypeStruct((tp_count, w_output.shape[1] // HD * taken + TAIL, HD), BF16),
        [VMEM] * 2,
        2 * tokens * w_output.size,
        4 * w_output.size,
        [pltpu.VMEM((16, w_output.shape[0]), F32)],
        "deliver",
    )(mix, w_output)
    shares = lax.all_to_all(shares, "tp", 0, 0, tiled=True)
    return call(
        settle,
        (
            jax.ShapeDtypeStruct((taken, w_output.shape[1]), BF16),
            jax.ShapeDtypeStruct((steps, w_output.shape[1]), BF16),
        ),
        [VMEM],
        2 * tokens * w_output.shape[1],
        2 * tokens * w_output.shape[1],
        name="settle",
    )(shares)


def solution(mesh):
    in_specs = (
        P("groups", "kv"),
        P("groups", "kv"),
        P("kv"),
        P("kv", "tp"),
        P("kv", "tp"),
        P("kv", "tp"),
        P("tp", "kv"),
        P("groups", "kv", "tp"),
        P("groups"),
        P("groups"),
        P("groups"),
        P("groups"),
    )
    out_specs = (P(("groups", "tp"), "kv"), P("groups", "kv"))
    return jax.shard_map(
        on_device, mesh=mesh, in_specs=in_specs, out_specs=out_specs, check_vma=False
    )
```

```python
import functools
import math

import jax
import jax.numpy as jnp
from jax import lax
from jax.experimental import pallas as pl
from jax.experimental.pallas import tpu as pltpu
from jax.sharding import PartitionSpec as P

HD = 128
SEQS = 2
EPSILON = 1e-05
THETA = 500000.0
NEGATIVE = -1e30
TAIL = 8
F32 = jnp.float32
BF16 = jnp.bfloat16
VMEM = pltpu.VMEM
SMEM = pltpu.SMEM
HBM = pltpu.HBM


def call(body, outs, spaces, flops, traffic, scratch=(), name=None, limit=20 << 20):
    return pl.pallas_call(
        body,
        out_shape=outs,
        in_specs=[pl.BlockSpec(memory_space=s) for s in spaces],
        out_specs=jax.tree.map(lambda _: pl.BlockSpec(memory_space=VMEM), outs),
        scratch_shapes=list(scratch),
        compiler_params=pltpu.CompilerParams(vmem_limit_bytes=limit),
        cost_estimate=pl.CostEstimate(flops=flops, bytes_accessed=traffic, transcendentals=0),
        name=name,
    )


def two_terms(value):
    high = value.astype(BF16).astype(F32)
    return high, value - high


def three_terms(value):
    high, rest = two_terms(value)
    mid, low = two_terms(rest)
    return high, mid, low


def stacked_rows(rows):
    place = lax.broadcasted_iota(jnp.int32, (TAIL, HD), 0)
    block = jnp.zeros((TAIL, HD), F32)
    for k, row in enumerate(rows):
        block = jnp.where(place == k, jnp.broadcast_to(row, (TAIL, HD)), block)
    return block


def turned(values, cosines, sines):
    half = HD // 2
    swapped = jnp.concatenate([values[:, half:], values[:, :half]], axis=1)
    return values * cosines + swapped * sines


def project(
    prompt_in, step_in, gain_in, query_in, key_in, value_in, own, above, below,
    prompt, step_pad, gain, w_query, w_pair, sems,
):
    near = own.shape[0]
    part_count = above.shape[0]
    count = 2 * near
    share = prompt.shape[0] // count
    heads = w_query.shape[1] // HD
    steps = step_in.shape[0]
    half = key_in.shape[0]
    parity = lax.rem(lax.axis_index("kv"), 2)
    pairs = [
        (gain_in, gain),
        (query_in, w_query),
        (step_in, step_pad),
        (key_in, w_pair.at[0:half, :]),
        (value_in, w_pair.at[half : 2 * half, :]),
    ]
    for k in range(count):
        chunk = 2 * k + parity if k < near else 2 * (k - near) + 1 - parity
        pairs.append(
            (
                prompt_in.at[pl.ds(pl.multiple_of(chunk * share, share), share), :],
                prompt.at[k * share : (k + 1) * share, :],
            )
        )
    moves = [
        pltpu.make_async_copy(source, target, sems.at[k])
        for k, (source, target) in enumerate(pairs)
    ]
    for move in moves[5:] + moves[:5]:
        move.start()
    for move in moves[5:]:
        move.wait()
    moves[0].wait()
    wide = prompt[...].astype(F32)
    scale = gain[...].astype(F32).reshape(1, gain.shape[0])
    normed = (wide * scale).astype(BF16)
    square = wide * wide
    high, low = two_terms(square)
    ones = jnp.ones((TAIL, prompt.shape[1]), BF16)
    dims = (((1,), (1,)), ((), ()))
    sums = lax.dot_general(ones, high.astype(BF16), dims, preferred_element_type=F32)
    sums = sums + lax.dot_general(ones, low.astype(BF16), dims, preferred_element_type=F32)
    sums = sums[0:1, :]
    moves[2].wait()
    step_wide = jnp.concatenate(
        [step_pad[...].astype(F32), jnp.zeros((TAIL - steps, prompt.shape[1]), F32)], axis=0
    )
    step_normed = (step_wide * scale).astype(BF16)
    step_sums = jnp.sum(step_wide * step_wide, axis=1, keepdims=True)

    def put(c, part):
        at = slice(c * share, (c + 1) * share)
        cut, end = near * share, (near + part_count) * share
        own[:, at, :] = part[:cut, :].reshape(near, share, HD)
        above[:, at, :] = part[cut:end, :].reshape(part_count, share, HD).astype(BF16)
        below[:, at, :] = part[end:, :].reshape(near - part_count, share, HD).astype(BF16)

    step_pieces = []
    moves[1].wait()
    for c in range(0, heads, 2):
        weight = w_query[:, c * HD : (c + 2) * HD]
        part = jnp.dot(normed, weight, preferred_element_type=F32)
        put(c, part[:, :HD])
        put(c + 1, part[:, HD:])
        small = jnp.dot(step_normed, weight, preferred_element_type=F32)
        step_pieces += [small[:, :HD], small[:, HD:]]
    moves[3].wait()
    moves[4].wait()
    put(heads, lax.dot_general(normed, w_pair[...], dims, preferred_element_type=F32))
    step_pieces.append(
        lax.dot_general(step_normed, w_pair[...], dims, preferred_element_type=F32)
    )

    def step_part(d):
        s, c = divmod(d, heads + 1)
        if s >= steps:
            return jnp.zeros((1, HD), F32), jnp.zeros((1, HD), F32)
        return step_pieces[c][s : s + 1, :], jnp.broadcast_to(step_sums[s : s + 1, :], (1, HD))

    start = (heads + 1) * share
    for k in range(count):
        lane = k * share // HD * HD
        even, odd = step_part(k % near * 2), step_part(k % near * 2 + 1)
        if k >= near:
            even, odd = odd, even
        piece, total = (jnp.where(parity == 0, a, b) for a, b in zip(even, odd))
        tail = stacked_rows([piece, *two_terms(sums[:, lane : lane + HD]), *two_terms(total)])
        if k < near:
            own[k, start : start + TAIL, :] = tail
        elif k < near + part_count:
            above[k - near, start : start + TAIL, :] = tail.astype(BF16)
        else:
            below[k - near - part_count, start : start + TAIL, :] = tail.astype(BF16)


def merge(own, under, over, out):
    near, size, _ = own.shape
    start = size - TAIL
    for k in range(near):
        other = under[k] if k < under.shape[0] else over[k - under.shape[0]]
        both = own[k] + other.astype(F32)
        out[k, 0:start, :] = both[:start, :].astype(BF16)
        tail = both[start:, :]
        out[k, start:, :] = stacked_rows(
            [
                tail[0:1, :],
                *two_terms(tail[1:2, :] + tail[2:3, :]),
                *two_terms(tail[3:4, :] + tail[4:5, :]),
            ]
        ).astype(BF16)


def complete(where, tiles, cosines, sines, out, *, features):
    count = tiles.shape[0]
    share = cosines.shape[0] - TAIL
    heads = (out.shape[0] - 3 * TAIL) // share - 2

    def total(start, size):
        return jnp.sum(tiles[:, start : start + size, :].astype(F32), axis=0)

    tail = total((heads + 1) * share, TAIL)
    row_scale = lax.rsqrt((tail[1:2, :] + tail[2:3, :]) / features + EPSILON)
    offset = lax.rem(where[0] // 2 * share, HD)
    place = lax.broadcasted_iota(jnp.int32, (share, HD), 0) + offset
    lane = lax.broadcasted_iota(jnp.int32, (share, HD), 1)
    scale = jnp.sum(
        jnp.where(place == lane, jnp.broadcast_to(row_scale, (share, HD)), 0.0),
        axis=1,
        keepdims=True,
    )
    step_scale = lax.rsqrt((tail[3:4, :] + tail[4:5, :]) / features + EPSILON)
    first = lax.broadcasted_iota(jnp.int32, (TAIL, HD), 0) == 0
    step_value = jnp.where(first, jnp.broadcast_to(tail[0:1, :] * step_scale, (TAIL, HD)), 0.0)
    cosine, sine = cosines[0:share, :], sines[0:share, :]
    for c in range(heads):
        value = total(c * share, share) * scale
        out[c * share : (c + 1) * share, :] = turned(value, cosine, sine).astype(BF16)
    out[heads * share : heads * share + TAIL, :] = turned(
        step_value, cosines[share:, :], sines[share:, :]
    ).astype(BF16)
    at = heads * share + TAIL
    for high_low in zip(two_terms(total(heads * share, share) * scale), two_terms(step_value)):
        out[at : at + share, :] = high_low[0].astype(BF16)
        out[at + share : at + share + TAIL, :] = high_low[1].astype(BF16)
        at += share + TAIL


def attend(
    where,
    starts,
    slots,
    offsets,
    lengths,
    queries,
    own_part,
    other_part,
    cosines,
    sines,
    cache_in,
    out,
    own_keys,
    own_values,
    step_query,
    values,
    bias,
    cache,
    sems,
    *,
    group,
):
    count = queries.shape[0]
    share = cosines.shape[0] - TAIL
    heads = (queries.shape[1] - TAIL) // share
    rows = heads * share
    members = slots.shape[0]
    steps = lengths.shape[0]
    block = cache.shape[1]
    half = HD // 2
    moves = [
        pltpu.make_async_copy(
            cache_in.at[SEQS + slots[k] if k < members else k - members],
            cache.at[k],
            sems.at[k],
        )
        for k in range(members + steps)
    ]
    for move in moves:
        move.start()
    mine = where[0]
    first = where[1] == 0
    base2 = math.log2(math.e)
    root = base2 / math.sqrt(HD)

    def pair_of(part):
        at = rows + TAIL
        high = part[at : at + share + TAIL, :].astype(F32)
        return high + part[at + share + TAIL : at + 2 * (share + TAIL), :].astype(F32)

    own_pair, other_pair = pair_of(own_part), pair_of(other_part)
    low_half = jnp.where(first, own_pair, other_pair)
    high_half = jnp.where(first, other_pair, own_pair)
    raw_keys = jnp.concatenate([low_half[:, :half], high_half[:, :half]], axis=1)
    raw_values = jnp.concatenate([low_half[:, half:], high_half[:, half:]], axis=1)
    own_keys[...] = turned(raw_keys, cosines[...], sines[...])
    own_values[...] = jnp.zeros_like(own_values)
    own_values[0 : share + TAIL, :] = raw_values
    keys_here = own_keys[0:share, :].astype(BF16)
    values_here = jnp.transpose(own_values[...])[:, 0:share].astype(BF16)
    dims = (((1,), (1,)), ((), ()))
    key_place = lax.broadcasted_iota(jnp.int32, (1, block), 1) + mine * block
    tile = group * rows
    lane = lax.broadcasted_iota(jnp.int32, (share, tile), 1)
    token_in_tile = lane // rows * share + lax.rem(lane, share)
    key_token = mine * share + lax.broadcasted_iota(jnp.int32, (share, tile), 0)

    key_column = lax.broadcasted_iota(jnp.int32, (block, HD), 0) + mine * block
    for r in range(members):
        moves[r].wait()
        for k in range(0, block, HD):
            values[r, :, k : k + HD] = jnp.transpose(
                cache[r, k : k + HD, HD:].astype(F32)
            ).astype(BF16)
        bias[r] = jnp.where(key_column < offsets[r], 0.0, NEGATIVE)

    step_rows = {}
    for s in range(steps):
        moves[members + s].wait()
        step_query[...] = jnp.zeros_like(step_query)
        for h in range(heads):
            step_query[h : h + 1, :] = queries[s * (heads + 1) + h, rows : rows + TAIL, :].astype(
                F32
            )[0:1, :]
        query = step_query[...]
        scores = lax.dot_general(
            query.astype(BF16), cache[members + s, :, 0:HD], dims, preferred_element_type=F32
        ) * root + jnp.where(key_place < lengths[s], 0.0, NEGATIVE)
        own_key = own_keys[share : share + 1, :].astype(BF16).astype(F32)
        own_value = own_values[share : share + 1, :].astype(BF16).astype(F32)
        own = jnp.sum(query * own_key, axis=1, keepdims=True) * root
        own = jnp.where(mine == s * (heads + 1) + heads, own, NEGATIVE)
        top = jnp.maximum(jnp.max(scores, axis=1, keepdims=True), own)
        weights = jnp.exp2(scores - top)
        own_weight = jnp.exp2(own - top)
        denominator = jnp.sum(weights, axis=1, keepdims=True) + own_weight
        mixed = jnp.dot(weights.astype(BF16), cache[members + s, :, HD:], preferred_element_type=F32)
        mixed = mixed + own_weight.astype(BF16).astype(F32) * own_value
        mixed = mixed / denominator
        level = top + jnp.log(denominator) * base2
        for h in range(heads):
            step_rows[s * heads + h] = [mixed[h : h + 1, :]] + [
                jnp.broadcast_to(t, (1, HD)) for t in three_terms(level[h : h + 1, :])
            ]

    for t in range(count // group):
        begin = t * group * share
        token = token_in_tile + begin
        query = queries[t * group : (t + 1) * group, 0:rows, :].reshape(tile, HD)

        for r in range(members):
            since = starts[r]
            until = starts[r + 1]

            @pl.when((since < begin + group * share) & (until > begin))
            def _():
                scored = lax.dot_general(keys_here, query, dims, preferred_element_type=F32)
                own = jnp.where((key_token >= since) & (key_token <= token), scored, NEGATIVE)
                limit = jnp.concatenate([bias[r]] * (tile // HD), axis=1)
                scores = (
                    lax.dot_general(
                        cache[r, :, 0:HD], query, dims, preferred_element_type=F32
                    )
                    + limit
                )
                top = jnp.maximum(
                    jnp.max(scores, axis=0, keepdims=True), jnp.max(own, axis=0, keepdims=True)
                )
                weights = jnp.exp2((scores - top) * root)
                own_weights = jnp.exp2((own - top) * root)
                denominator = jnp.sum(weights, axis=0, keepdims=True) + jnp.sum(
                    own_weights, axis=0, keepdims=True
                )
                mixed = jnp.dot(values[r], weights.astype(BF16), preferred_element_type=F32)
                mixed = mixed + jnp.dot(
                    values_here, own_weights.astype(BF16), preferred_element_type=F32
                )
                mixed = mixed / denominator
                level = top * root + jnp.log(denominator) * base2
                for g in range(group):
                    d = t * group + g
                    piece = mixed[:, g * rows : (g + 1) * rows]
                    flat = level[:, g * rows : (g + 1) * rows]
                    tail = stacked_rows(list(three_terms(flat)) + step_rows.get(d, []))

                    @pl.when(since <= begin + g * share)
                    def _():
                        out[d, 0:HD, :] = piece.astype(BF16)
                        out[d, HD : HD + TAIL, :] = tail.astype(BF16)

                    @pl.when(since > begin + g * share)
                    def _():
                        late = token[:, g * rows : (g + 1) * rows][0:1, :] >= since
                        before = out[d, 0:HD, :].astype(F32)
                        out[d, 0:HD, :] = jnp.where(late, piece, before).astype(BF16)
                        earlier = out[d, HD : HD + TAIL, :].astype(F32)
                        out[d, HD : HD + TAIL, :] = jnp.where(late, tail, earlier).astype(BF16)


def combine(tiles, out):
    rows = tiles.shape[2]
    tail = tiles[:, HD : HD + TAIL, :].astype(F32)

    def shares(at):
        level = tail[:, at, :] + tail[:, at + 1, :] + tail[:, at + 2, :]
        weight = jnp.exp2(level - jnp.max(level, axis=0, keepdims=True))
        return weight / jnp.sum(weight, axis=0, keepdims=True)

    weight = shares(0)
    mixed = jnp.zeros((HD, rows), F32)
    for k in range(tiles.shape[0]):
        mixed = mixed + weight[k : k + 1, :] * tiles[k, 0:HD, :].astype(F32)
    out[0:rows, :] = jnp.transpose(mixed).astype(BF16)
    step = jnp.sum(shares(4) * tail[:, 3, :], axis=0, keepdims=True)
    out[rows : rows + TAIL, :] = jnp.broadcast_to(step, (TAIL, HD)).astype(BF16)


def deliver(where, mix, w_here, w_there, out, step_pad, *, steps):
    count = mix.shape[0]
    heads = w_here.shape[0] // HD
    share = (mix.shape[1] - TAIL) // heads
    takers = out.shape[0]
    wide = w_here.shape[1] // HD
    taken = count * share // takers
    step_pad[...] = jnp.zeros_like(step_pad)
    for s in range(steps):
        for h in range(heads):
            step_pad[s : s + 1, h * HD : (h + 1) * HD] = mix[
                s * heads + h, heads * share : heads * share + TAIL, :
            ].astype(F32)[0:1, :]

    def project_with(w_output):
        block = jnp.concatenate(
            [
                mix[:, h * share : (h + 1) * share, :].reshape(count * share, HD)
                for h in range(heads)
            ],
            axis=1,
        )
        small = jnp.dot(step_pad[...].astype(BF16), w_output[...], preferred_element_type=F32)
        tail = stacked_rows(
            [small[s : s + 1, c * HD : (c + 1) * HD] for s in range(steps) for c in range(wide)]
        ).astype(BF16)
        for c in range(0, wide, 2):
            part = jnp.dot(
                block, w_output[:, c * HD : (c + 2) * HD], preferred_element_type=F32
            ).astype(BF16)
            for k in range(2):
                out[:, (c + k) * taken : (c + k + 1) * taken, :] = part[
                    :, k * HD : (k + 1) * HD
                ].reshape(takers, taken, HD)
        for d in range(takers):
            out[d, wide * taken : wide * taken + TAIL, :] = tail

    pl.when(lax.rem(where[0], 2) == 0)(lambda: project_with(w_here))
    pl.when(lax.rem(where[0], 2) == 1)(lambda: project_with(w_there))


def settle(tiles, prompt_out, step_out):
    taken, width = prompt_out.shape
    wide = width // HD
    for c in range(wide):
        prompt_out[:, c * HD : (c + 1) * HD] = jnp.sum(
            tiles[:, c * taken : (c + 1) * taken, :].astype(F32), axis=0
        ).astype(BF16)
    tail = jnp.sum(tiles[:, wide * taken : wide * taken + TAIL, :].astype(F32), axis=0)
    for s in range(step_out.shape[0]):
        for c in range(wide):
            step_out[s : s + 1, c * HD : (c + 1) * HD] = tail[
                s * wide + c : s * wide + c + 1, :
            ].astype(BF16)


def on_device(
    prompt_rows,
    step_rows,
    norm_gain,
    w_query,
    w_key,
    w_value,
    w_output,
    kv_cache,
    step_lengths,
    rollout_ids,
    resume_offsets,
    stretch_rollout,
):
    kv_index = lax.axis_index("kv")
    kv_count = lax.axis_size("kv")
    tp_index = lax.axis_index("tp")
    tp_count = lax.axis_size("tp")
    tokens, width = prompt_rows.shape
    steps = step_rows.shape[0]
    heads = w_query.shape[1] // HD
    share = tokens // kv_count
    taken = tokens // tp_count
    rows = heads * share
    members = resume_offsets.shape[0]
    where = jnp.stack([kv_index, lax.rem(tp_index, 2)]).astype(jnp.int32)

    swap = [(k, k ^ 1) for k in range(tp_count)]
    lines = [
        [(pair * 2 + (core ^ (z & 1))) * kv_count + z for z in range(kv_count)]
        for pair in range(tp_count // 2)
        for core in range(2)
    ]

    both = ("tp", "kv")
    near = kv_count // 2
    size = rows + share + TAIL

    def shifted(value, step):
        return lax.ppermute(
            value, "kv", [(z, (z + step) % kv_count) for z in range(kv_count)]
        )

    own, above, below = call(
        project,
        (
            jax.ShapeDtypeStruct((near, size, HD), F32),
            jax.ShapeDtypeStruct((near // 2, size, HD), BF16),
            jax.ShapeDtypeStruct((near - near // 2, size, HD), BF16),
        ),
        [HBM] * 6,
        2 * tokens * width * (w_query.shape[1] + HD),
        4 * tokens * width,
        [
            pltpu.VMEM((tokens, width), BF16),
            pltpu.VMEM((steps, width), BF16),
            pltpu.VMEM((width,), BF16),
            pltpu.VMEM(w_query.shape, BF16),
            pltpu.VMEM((HD, width), BF16),
            pltpu.SemaphoreType.DMA((5 + kv_count,)),
        ],
        "project",
        limit=60 << 20,
    )(prompt_rows, step_rows, norm_gain, w_query, w_key.T, w_value.T)
    own, w_output = lax.optimization_barrier((own, w_output))
    w_output_there = lax.ppermute(w_output, "tp", swap)
    parts = call(
        merge,
        jax.ShapeDtypeStruct((near, size, HD), BF16),
        [VMEM] * 3,
        near * size * HD,
        8 * near * size * HD,
        name="merge",
    )(own, shifted(above, 1), shifted(below, -1))
    strides = [
        [t * kv_count + z for z in range(parity, kv_count, 2)]
        for t in range(tp_count)
        for parity in range(2)
    ]
    parts = lax.all_to_all(parts, both, 0, 0, tiled=True, axis_index_groups=strides)

    member_index = jnp.arange(members + 1, dtype=jnp.int32)
    starts = jnp.sum(
        (stretch_rollout[:, None] < member_index[None, :]).astype(jnp.int32), axis=0
    )
    tokens_here = kv_index * share + jnp.arange(share, dtype=jnp.int32)
    rollout_here = jnp.sum(
        (tokens_here[:, None] >= starts[None, 1:members]).astype(jnp.int32), axis=1
    )
    onehot = (rollout_here[:, None] == member_index[None, :members]).astype(jnp.int32)
    positions = jnp.sum(onehot * (resume_offsets - starts[:members])[None, :], axis=1) + tokens_here
    step_place = jnp.minimum(kv_index // (heads + 1), steps - 1)
    step_position = lax.dynamic_slice_in_dim(step_lengths, step_place, 1, 0)
    positions = jnp.concatenate([positions, jnp.broadcast_to(step_position, (TAIL,))])
    half = HD // 2
    inverse = jnp.exp(jnp.arange(half, dtype=F32) * (-2.0 * math.log(THETA) / HD))
    angles = positions.astype(F32)[:, None] * inverse[None, :]
    cosine, sine = jnp.cos(angles), jnp.sin(angles)
    cosines = jnp.concatenate([cosine, cosine], axis=1)
    sines = jnp.concatenate([-sine, sine], axis=1)

    block = kv_cache.shape[1]
    here = call(
        functools.partial(complete, features=width * kv_count),
        jax.ShapeDtypeStruct((rows + TAIL + 2 * (share + TAIL), HD), BF16),
        [SMEM] + [VMEM] * 3,
        2 * kv_count * rows * HD,
        2 * kv_count * rows * HD,
        name="complete",
    )(where, parts, cosines, sines)
    there = lax.ppermute(here, "tp", swap)
    query_here = jnp.where(
        lax.rem(kv_index, 2) == 0, here[: rows + TAIL], there[: rows + TAIL]
    )
    queries = lax.all_gather(query_here, both, axis=0, axis_index_groups=lines)

    mixed = call(
        functools.partial(attend, group=4),
        jax.ShapeDtypeStruct((kv_count, HD + TAIL, rows), BF16),
        [SMEM] * 5 + [VMEM] * 5 + [HBM],
        4 * tokens * heads * block * HD,
        kv_cache.size,
        [
            pltpu.VMEM((share + TAIL, HD), F32),
            pltpu.VMEM((HD, HD), F32),
            pltpu.VMEM((16, HD), F32),
            pltpu.VMEM((members, HD, block), BF16),
            pltpu.VMEM((members, block, HD), F32),
            pltpu.VMEM((members + steps, block, 2 * HD), BF16),
            pltpu.SemaphoreType.DMA((members + steps,)),
        ],
        "attend",
        limit=58 << 20,
    )(
        where,
        starts,
        rollout_ids,
        resume_offsets,
        step_lengths,
        queries,
        here,
        there,
        cosines,
        sines,
        kv_cache,
    )
    mixed = lax.all_to_all(mixed, both, 0, 0, tiled=True, axis_index_groups=lines)
    mix_here = call(
        combine,
        jax.ShapeDtypeStruct((rows + TAIL, HD), BF16),
        [VMEM],
        2 * kv_count * rows * HD,
        2 * kv_count * rows * HD,
        name="combine",
    )(mixed)
    mix = lax.all_gather(mix_here, both, axis=0, axis_index_groups=lines)
    shares = call(
        functools.partial(deliver, steps=steps),
        jax.ShapeDtypeStruct((tp_count, w_output.shape[1] // HD * taken + TAIL, HD), BF16),
        [SMEM] + [VMEM] * 3,
        2 * tokens * w_output.size,
        4 * w_output.size,
        [pltpu.VMEM((16, w_output.shape[0]), F32)],
        "deliver",
    )(where, mix, w_output, w_output_there)
    shares = lax.all_to_all(shares, "tp", 0, 0, tiled=True)
    return call(
        settle,
        (
            jax.ShapeDtypeStruct((taken, w_output.shape[1]), BF16),
            jax.ShapeDtypeStruct((steps, w_output.shape[1]), BF16),
        ),
        [VMEM],
        2 * tokens * w_output.shape[1],
        2 * tokens * w_output.shape[1],
        name="settle",
    )(shares)


def solution(mesh):
    in_specs = (
        P("groups", "kv"),
        P("groups", "kv"),
        P("kv"),
        P("kv", "tp"),
        P("kv", "tp"),
        P("kv", "tp"),
        P("tp", "kv"),
        P("groups", "kv", "tp"),
        P("groups"),
        P("groups"),
        P("groups"),
        P("groups"),
    )
    out_specs = (P(("groups", "tp"), "kv"), P("groups", "kv"))
    return jax.shard_map(
        on_device, mesh=mesh, in_specs=in_specs, out_specs=out_specs, check_vma=False
    )
```

```python
import functools
import math

import jax
import jax.numpy as jnp
from jax import lax
from jax.experimental import pallas as pl
from jax.experimental.pallas import tpu as pltpu
from jax.sharding import PartitionSpec as P

HD = 128
SEQS = 2
EPSILON = 1e-05
THETA = 500000.0
NEGATIVE = -1e30
TAIL = 8
F32 = jnp.float32
BF16 = jnp.bfloat16
VMEM = pltpu.VMEM
SMEM = pltpu.SMEM
HBM = pltpu.HBM


def call(body, outs, spaces, flops, traffic, scratch=(), name=None, limit=20 << 20):
    return pl.pallas_call(
        body,
        out_shape=outs,
        in_specs=[pl.BlockSpec(memory_space=s) for s in spaces],
        out_specs=jax.tree.map(lambda _: pl.BlockSpec(memory_space=VMEM), outs),
        scratch_shapes=list(scratch),
        compiler_params=pltpu.CompilerParams(vmem_limit_bytes=limit),
        cost_estimate=pl.CostEstimate(flops=flops, bytes_accessed=traffic, transcendentals=0),
        name=name,
    )


def two_terms(value):
    high = value.astype(BF16).astype(F32)
    return high, value - high


def three_terms(value):
    high, rest = two_terms(value)
    mid, low = two_terms(rest)
    return high, mid, low


def stacked_rows(rows):
    place = lax.broadcasted_iota(jnp.int32, (TAIL, HD), 0)
    block = jnp.zeros((TAIL, HD), F32)
    for k, row in enumerate(rows):
        block = jnp.where(place == k, jnp.broadcast_to(row, (TAIL, HD)), block)
    return block


def turned(values, cosines, sines):
    half = HD // 2
    swapped = jnp.concatenate([values[:, half:], values[:, :half]], axis=1)
    return values * cosines + swapped * sines


def project(
    prompt_in, step_in, gain_in, query_in, key_in, value_in, own, above, below,
    prompt, step_pad, gain, w_query, w_pair, sems,
):
    near = own.shape[0]
    part_count = above.shape[0]
    count = 2 * near
    share = prompt.shape[0] // count
    heads = w_query.shape[1] // HD
    steps = step_in.shape[0]
    half = key_in.shape[0]
    parity = lax.rem(lax.axis_index("kv"), 2)
    pairs = [
        (gain_in, gain),
        (query_in, w_query),
        (step_in, step_pad),
        (key_in, w_pair.at[0:half, :]),
        (value_in, w_pair.at[half : 2 * half, :]),
    ]
    for k in range(count):
        chunk = 2 * k + parity if k < near else 2 * (k - near) + 1 - parity
        pairs.append(
            (
                prompt_in.at[pl.ds(pl.multiple_of(chunk * share, share), share), :],
                prompt.at[k * share : (k + 1) * share, :],
            )
        )
    moves = [
        pltpu.make_async_copy(source, target, sems.at[k])
        for k, (source, target) in enumerate(pairs)
    ]
    for move in moves[5:] + moves[:5]:
        move.start()
    for move in moves[5:]:
        move.wait()
    moves[0].wait()
    wide = prompt[...].astype(F32)
    scale = gain[...].astype(F32).reshape(1, gain.shape[0])
    normed = (wide * scale).astype(BF16)
    square = wide * wide
    high, low = two_terms(square)
    ones = jnp.ones((TAIL, prompt.shape[1]), BF16)
    dims = (((1,), (1,)), ((), ()))
    sums = lax.dot_general(ones, high.astype(BF16), dims, preferred_element_type=F32)
    sums = sums + lax.dot_general(ones, low.astype(BF16), dims, preferred_element_type=F32)
    sums = sums[0:1, :]
    moves[2].wait()
    step_wide = jnp.concatenate(
        [step_pad[...].astype(F32), jnp.zeros((TAIL - steps, prompt.shape[1]), F32)], axis=0
    )
    step_normed = (step_wide * scale).astype(BF16)
    step_sums = jnp.sum(step_wide * step_wide, axis=1, keepdims=True)

    def put(c, part):
        at = slice(c * share, (c + 1) * share)
        cut, end = near * share, (near + part_count) * share
        own[:, at, :] = part[:cut, :].reshape(near, share, HD)
        above[:, at, :] = part[cut:end, :].reshape(part_count, share, HD).astype(BF16)
        below[:, at, :] = part[end:, :].reshape(near - part_count, share, HD).astype(BF16)

    step_pieces = []
    moves[1].wait()
    for c in range(0, heads, 2):
        weight = w_query[:, c * HD : (c + 2) * HD]
        part = jnp.dot(normed, weight, preferred_element_type=F32)
        put(c, part[:, :HD])
        put(c + 1, part[:, HD:])
        small = jnp.dot(step_normed, weight, preferred_element_type=F32)
        step_pieces += [small[:, :HD], small[:, HD:]]
    moves[3].wait()
    moves[4].wait()
    put(heads, lax.dot_general(normed, w_pair[...], dims, preferred_element_type=F32))
    step_pieces.append(
        lax.dot_general(step_normed, w_pair[...], dims, preferred_element_type=F32)
    )

    def step_part(d):
        s, c = divmod(d, heads + 1)
        if s >= steps:
            return jnp.zeros((1, HD), F32), jnp.zeros((1, HD), F32)
        return step_pieces[c][s : s + 1, :], jnp.broadcast_to(step_sums[s : s + 1, :], (1, HD))

    start = (heads + 1) * share
    for k in range(count):
        lane = k * share // HD * HD
        even, odd = step_part(k % near * 2), step_part(k % near * 2 + 1)
        if k >= near:
            even, odd = odd, even
        piece, total = (jnp.where(parity == 0, a, b) for a, b in zip(even, odd))
        tail = stacked_rows([piece, *two_terms(sums[:, lane : lane + HD]), *two_terms(total)])
        if k < near:
            own[k, start : start + TAIL, :] = tail
        elif k < near + part_count:
            above[k - near, start : start + TAIL, :] = tail.astype(BF16)
        else:
            below[k - near - part_count, start : start + TAIL, :] = tail.astype(BF16)


def merge(own, under, over, out):
    near, size, _ = own.shape
    start = size - TAIL
    for k in range(near):
        other = under[k] if k < under.shape[0] else over[k - under.shape[0]]
        both = own[k] + other.astype(F32)
        out[k, 0:start, :] = both[:start, :].astype(BF16)
        tail = both[start:, :]
        out[k, start:, :] = stacked_rows(
            [
                tail[0:1, :],
                *two_terms(tail[1:2, :] + tail[2:3, :]),
                *two_terms(tail[3:4, :] + tail[4:5, :]),
            ]
        ).astype(BF16)


def complete(where, tiles, cosines, sines, out, *, features):
    count = tiles.shape[0]
    share = cosines.shape[0] - TAIL
    heads = (out.shape[0] - 3 * TAIL) // share - 2

    def total(start, size):
        return jnp.sum(tiles[:, start : start + size, :].astype(F32), axis=0)

    tail = total((heads + 1) * share, TAIL)
    row_scale = lax.rsqrt((tail[1:2, :] + tail[2:3, :]) / features + EPSILON)
    offset = lax.rem(where[0] // 2 * share, HD)
    place = lax.broadcasted_iota(jnp.int32, (share, HD), 0) + offset
    lane = lax.broadcasted_iota(jnp.int32, (share, HD), 1)
    scale = jnp.sum(
        jnp.where(place == lane, jnp.broadcast_to(row_scale, (share, HD)), 0.0),
        axis=1,
        keepdims=True,
    )
    step_scale = lax.rsqrt((tail[3:4, :] + tail[4:5, :]) / features + EPSILON)
    first = lax.broadcasted_iota(jnp.int32, (TAIL, HD), 0) == 0
    step_value = jnp.where(first, jnp.broadcast_to(tail[0:1, :] * step_scale, (TAIL, HD)), 0.0)
    cosine, sine = cosines[0:share, :], sines[0:share, :]
    for c in range(heads):
        value = total(c * share, share) * scale
        out[c * share : (c + 1) * share, :] = turned(value, cosine, sine).astype(BF16)
    out[heads * share : heads * share + TAIL, :] = turned(
        step_value, cosines[share:, :], sines[share:, :]
    ).astype(BF16)
    at = heads * share + TAIL
    for high_low in zip(two_terms(total(heads * share, share) * scale), two_terms(step_value)):
        out[at : at + share, :] = high_low[0].astype(BF16)
        out[at + share : at + share + TAIL, :] = high_low[1].astype(BF16)
        at += share + TAIL


def attend(
    where,
    starts,
    slots,
    offsets,
    lengths,
    queries,
    own_part,
    other_part,
    cosines,
    sines,
    cache_in,
    own_out,
    above_out,
    below_out,
    own_keys,
    own_values,
    step_query,
    values,
    bias,
    cache,
    out,
    sems,
    *,
    group,
):
    count = queries.shape[0]
    share = cosines.shape[0] - TAIL
    heads = (queries.shape[1] - TAIL) // share
    rows = heads * share
    members = slots.shape[0]
    steps = lengths.shape[0]
    block = cache.shape[1]
    half = HD // 2
    moves = [
        pltpu.make_async_copy(
            cache_in.at[SEQS + slots[k] if k < members else k - members],
            cache.at[k],
            sems.at[k],
        )
        for k in range(members + steps)
    ]
    for move in moves:
        move.start()
    mine = where[0]
    parity = lax.rem(mine, 2)
    first = where[1] == 0
    base2 = math.log2(math.e)
    root = base2 / math.sqrt(HD)

    def pair_of(part):
        at = rows + TAIL
        high = part[at : at + share + TAIL, :].astype(F32)
        return high + part[at + share + TAIL : at + 2 * (share + TAIL), :].astype(F32)

    own_pair, other_pair = pair_of(own_part), pair_of(other_part)
    low_half = jnp.where(first, own_pair, other_pair)
    high_half = jnp.where(first, other_pair, own_pair)
    raw_keys = jnp.concatenate([low_half[:, :half], high_half[:, :half]], axis=1)
    raw_values = jnp.concatenate([low_half[:, half:], high_half[:, half:]], axis=1)
    own_keys[...] = turned(raw_keys, cosines[...], sines[...])
    own_values[...] = jnp.zeros_like(own_values)
    own_values[0 : share + TAIL, :] = raw_values
    keys_here = own_keys[0:share, :].astype(BF16)
    values_here = jnp.transpose(own_values[...])[:, 0:share].astype(BF16)
    dims = (((1,), (1,)), ((), ()))
    key_place = lax.broadcasted_iota(jnp.int32, (1, block), 1) + mine * block
    tile = group * rows
    lane = lax.broadcasted_iota(jnp.int32, (share, tile), 1)
    token_in_tile = lane // rows * share + lax.rem(lane, share)
    key_token = mine * share + lax.broadcasted_iota(jnp.int32, (share, tile), 0)

    key_column = lax.broadcasted_iota(jnp.int32, (block, HD), 0) + mine * block
    for r in range(members):
        moves[r].wait()
        for k in range(0, block, HD):
            values[r, :, k : k + HD] = jnp.transpose(
                cache[r, k : k + HD, HD:].astype(F32)
            ).astype(BF16)
        bias[r] = jnp.where(key_column < offsets[r], 0.0, NEGATIVE)

    step_rows = {}
    for s in range(steps):
        moves[members + s].wait()
        step_query[...] = jnp.zeros_like(step_query)
        for h in range(heads):
            step_query[h : h + 1, :] = queries[s * (heads + 1) + h, rows : rows + TAIL, :].astype(
                F32
            )[0:1, :]
        query = step_query[...]
        scores = lax.dot_general(
            query.astype(BF16), cache[members + s, :, 0:HD], dims, preferred_element_type=F32
        ) * root + jnp.where(key_place < lengths[s], 0.0, NEGATIVE)
        own_key = own_keys[share : share + 1, :].astype(BF16).astype(F32)
        own_value = own_values[share : share + 1, :].astype(BF16).astype(F32)
        own = jnp.sum(query * own_key, axis=1, keepdims=True) * root
        own = jnp.where(mine == s * (heads + 1) + heads, own, NEGATIVE)
        top = jnp.maximum(jnp.max(scores, axis=1, keepdims=True), own)
        weights = jnp.exp2(scores - top)
        own_weight = jnp.exp2(own - top)
        denominator = jnp.sum(weights, axis=1, keepdims=True) + own_weight
        mixed = jnp.dot(weights.astype(BF16), cache[members + s, :, HD:], preferred_element_type=F32)
        mixed = mixed + own_weight.astype(BF16).astype(F32) * own_value
        mixed = mixed / denominator
        level = top + jnp.log(denominator) * base2
        for h in range(heads):
            step_rows[s * heads + h] = [mixed[h : h + 1, :]] + [
                jnp.broadcast_to(t, (1, HD)) for t in three_terms(level[h : h + 1, :])
            ]

    for t in range(count // group):
        begin = t * group * share
        token = token_in_tile + begin
        query = queries[t * group : (t + 1) * group, 0:rows, :].reshape(tile, HD)

        for r in range(members):
            since = starts[r]
            until = starts[r + 1]

            @pl.when((since < begin + group * share) & (until > begin))
            def _():
                scored = lax.dot_general(keys_here, query, dims, preferred_element_type=F32)
                own = jnp.where((key_token >= since) & (key_token <= token), scored, NEGATIVE)
                limit = jnp.concatenate([bias[r]] * (tile // HD), axis=1)
                scores = (
                    lax.dot_general(
                        cache[r, :, 0:HD], query, dims, preferred_element_type=F32
                    )
                    + limit
                )
                top = jnp.maximum(
                    jnp.max(scores, axis=0, keepdims=True), jnp.max(own, axis=0, keepdims=True)
                )
                weights = jnp.exp2((scores - top) * root)
                own_weights = jnp.exp2((own - top) * root)
                denominator = jnp.sum(weights, axis=0, keepdims=True) + jnp.sum(
                    own_weights, axis=0, keepdims=True
                )
                mixed = jnp.dot(values[r], weights.astype(BF16), preferred_element_type=F32)
                mixed = mixed + jnp.dot(
                    values_here, own_weights.astype(BF16), preferred_element_type=F32
                )
                mixed = mixed / denominator
                level = top * root + jnp.log(denominator) * base2
                for g in range(group):
                    d = t * group + g
                    at = d // 2 + jnp.where(parity == d % 2, 0, count // 2)
                    piece = mixed[:, g * rows : (g + 1) * rows]
                    flat = level[:, g * rows : (g + 1) * rows]
                    tail = stacked_rows(list(three_terms(flat)) + step_rows.get(d, []))

                    @pl.when(since <= begin + g * share)
                    def _():
                        out[at, 0:HD, :] = piece.astype(BF16)
                        out[at, HD : HD + TAIL, :] = tail.astype(BF16)

                    @pl.when(since > begin + g * share)
                    def _():
                        late = token[:, g * rows : (g + 1) * rows][0:1, :] >= since
                        before = out[at, 0:HD, :].astype(F32)
                        out[at, 0:HD, :] = jnp.where(late, piece, before).astype(BF16)
                        earlier = out[at, HD : HD + TAIL, :].astype(F32)
                        out[at, HD : HD + TAIL, :] = jnp.where(late, tail, earlier).astype(BF16)

    near, part_count = own_out.shape[0], above_out.shape[0]
    own_out[...] = out[0:near]
    above_out[...] = out[near : near + part_count]
    below_out[...] = out[near + part_count :]


def unite(own, under, over, out):
    for k in range(own.shape[0]):
        other = under[k] if k < under.shape[0] else over[k - under.shape[0]]
        one, two = own[k].astype(F32), other.astype(F32)
        tails = one[HD:, :], two[HD:, :]

        def shares(at):
            first, second = (t[at : at + 1] + t[at + 1 : at + 2] + t[at + 2 : at + 3] for t in tails)
            top = jnp.maximum(first, second)
            first, second = jnp.exp2(first - top), jnp.exp2(second - top)
            total = first + second
            return first / total, second / total, top + jnp.log(total) * math.log2(math.e)

        left, right, level = shares(0)
        out[k, 0:HD, :] = (one[:HD, :] * left + two[:HD, :] * right).astype(BF16)
        left, right, step_level = shares(4)
        step = tails[0][3:4] * left + tails[1][3:4] * right
        out[k, HD:, :] = stacked_rows(
            [*three_terms(level), step, *three_terms(step_level)]
        ).astype(BF16)


def combine(where, tiles, mine, out):
    count, _, rows = tiles.shape
    place = where[0] // 2
    tail = jnp.stack(
        [jnp.where(place == k, mine[HD:, :], tiles[k, HD:, :]).astype(F32) for k in range(count)]
    )

    def shares(at):
        level = tail[:, at, :] + tail[:, at + 1, :] + tail[:, at + 2, :]
        weight = jnp.exp2(level - jnp.max(level, axis=0, keepdims=True))
        return weight / jnp.sum(weight, axis=0, keepdims=True)

    weight = shares(0)
    mixed = jnp.zeros((HD, rows), F32)
    for k in range(count):
        tile = jnp.where(place == k, mine[0:HD, :], tiles[k, 0:HD, :])
        mixed = mixed + weight[k : k + 1, :] * tile.astype(F32)
    out[0:rows, :] = jnp.transpose(mixed).astype(BF16)
    step = jnp.sum(shares(4) * tail[:, 3, :], axis=0, keepdims=True)
    out[rows : rows + TAIL, :] = jnp.broadcast_to(step, (TAIL, HD)).astype(BF16)


def deliver(where, mix, w_here, w_there, out, step_pad, *, steps):
    count = mix.shape[0]
    heads = w_here.shape[0] // HD
    share = (mix.shape[1] - TAIL) // heads
    takers = out.shape[0]
    wide = w_here.shape[1] // HD
    taken = count * share // takers
    step_pad[...] = jnp.zeros_like(step_pad)
    for s in range(steps):
        for h in range(heads):
            step_pad[s : s + 1, h * HD : (h + 1) * HD] = mix[
                s * heads + h, heads * share : heads * share + TAIL, :
            ].astype(F32)[0:1, :]

    def project_with(w_output):
        block = jnp.concatenate(
            [
                mix[:, h * share : (h + 1) * share, :].reshape(count * share, HD)
                for h in range(heads)
            ],
            axis=1,
        )
        small = jnp.dot(step_pad[...].astype(BF16), w_output[...], preferred_element_type=F32)
        tail = stacked_rows(
            [small[s : s + 1, c * HD : (c + 1) * HD] for s in range(steps) for c in range(wide)]
        ).astype(BF16)
        for c in range(0, wide, 2):
            part = jnp.dot(
                block, w_output[:, c * HD : (c + 2) * HD], preferred_element_type=F32
            ).astype(BF16)
            for k in range(2):
                out[:, (c + k) * taken : (c + k + 1) * taken, :] = part[
                    :, k * HD : (k + 1) * HD
                ].reshape(takers, taken, HD)
        for d in range(takers):
            out[d, wide * taken : wide * taken + TAIL, :] = tail

    pl.when(lax.rem(where[0], 2) == 0)(lambda: project_with(w_here))
    pl.when(lax.rem(where[0], 2) == 1)(lambda: project_with(w_there))


def settle(where, tiles, mine, prompt_out, step_out):
    taken, width = prompt_out.shape
    wide = width // HD
    total = jnp.zeros(mine.shape, F32)
    for k in range(tiles.shape[0]):
        total = total + jnp.where(where[2] == k, mine[...], tiles[k]).astype(F32)
    for c in range(wide):
        prompt_out[:, c * HD : (c + 1) * HD] = total[c * taken : (c + 1) * taken, :].astype(BF16)
    start = wide * taken
    for s in range(step_out.shape[0]):
        for c in range(wide):
            at = start + s * wide + c
            step_out[s : s + 1, c * HD : (c + 1) * HD] = total[at : at + 1, :].astype(BF16)


def on_device(
    prompt_rows,
    step_rows,
    norm_gain,
    w_query,
    w_key,
    w_value,
    w_output,
    kv_cache,
    step_lengths,
    rollout_ids,
    resume_offsets,
    stretch_rollout,
):
    kv_index = lax.axis_index("kv")
    kv_count = lax.axis_size("kv")
    tp_index = lax.axis_index("tp")
    tp_count = lax.axis_size("tp")
    tokens, width = prompt_rows.shape
    steps = step_rows.shape[0]
    heads = w_query.shape[1] // HD
    share = tokens // kv_count
    taken = tokens // tp_count
    rows = heads * share
    members = resume_offsets.shape[0]
    where = jnp.stack([kv_index, lax.rem(tp_index, 2), tp_index]).astype(jnp.int32)

    swap = [(k, k ^ 1) for k in range(tp_count)]
    lines = [
        [(pair * 2 + (core ^ (z & 1))) * kv_count + z for z in range(kv_count)]
        for pair in range(tp_count // 2)
        for core in range(2)
    ]

    both = ("tp", "kv")
    near = kv_count // 2
    size = rows + share + TAIL

    def shifted(value, step):
        return lax.ppermute(
            value, "kv", [(z, (z + step) % kv_count) for z in range(kv_count)]
        )

    own, above, below = call(
        project,
        (
            jax.ShapeDtypeStruct((near, size, HD), F32),
            jax.ShapeDtypeStruct((near // 2, size, HD), BF16),
            jax.ShapeDtypeStruct((near - near // 2, size, HD), BF16),
        ),
        [HBM] * 6,
        2 * tokens * width * (w_query.shape[1] + HD),
        4 * tokens * width,
        [
            pltpu.VMEM((tokens, width), BF16),
            pltpu.VMEM((steps, width), BF16),
            pltpu.VMEM((width,), BF16),
            pltpu.VMEM(w_query.shape, BF16),
            pltpu.VMEM((HD, width), BF16),
            pltpu.SemaphoreType.DMA((5 + kv_count,)),
        ],
        "project",
        limit=60 << 20,
    )(prompt_rows, step_rows, norm_gain, w_query, w_key.T, w_value.T)
    parts = call(
        merge,
        jax.ShapeDtypeStruct((near, size, HD), BF16),
        [VMEM] * 3,
        near * size * HD,
        8 * near * size * HD,
        name="merge",
    )(own, shifted(above, 1), shifted(below, -1))
    parts, w_output = lax.optimization_barrier((parts, w_output))
    w_output_there = lax.ppermute(w_output, "tp", swap)
    strides = [
        [t * kv_count + z for z in range(parity, kv_count, 2)]
        for t in range(tp_count)
        for parity in range(2)
    ]
    parts = lax.all_to_all(parts, both, 0, 0, tiled=True, axis_index_groups=strides)

    member_index = jnp.arange(members + 1, dtype=jnp.int32)
    starts = jnp.sum(
        (stretch_rollout[:, None] < member_index[None, :]).astype(jnp.int32), axis=0
    )
    tokens_here = kv_index * share + jnp.arange(share, dtype=jnp.int32)
    rollout_here = jnp.sum(
        (tokens_here[:, None] >= starts[None, 1:members]).astype(jnp.int32), axis=1
    )
    onehot = (rollout_here[:, None] == member_index[None, :members]).astype(jnp.int32)
    positions = jnp.sum(onehot * (resume_offsets - starts[:members])[None, :], axis=1) + tokens_here
    step_place = jnp.minimum(kv_index // (heads + 1), steps - 1)
    step_position = lax.dynamic_slice_in_dim(step_lengths, step_place, 1, 0)
    positions = jnp.concatenate([positions, jnp.broadcast_to(step_position, (TAIL,))])
    half = HD // 2
    inverse = jnp.exp(jnp.arange(half, dtype=F32) * (-2.0 * math.log(THETA) / HD))
    angles = positions.astype(F32)[:, None] * inverse[None, :]
    cosine, sine = jnp.cos(angles), jnp.sin(angles)
    cosines = jnp.concatenate([cosine, cosine], axis=1)
    sines = jnp.concatenate([-sine, sine], axis=1)

    block = kv_cache.shape[1]
    parts, w_output_there = lax.optimization_barrier((parts, w_output_there))
    here = call(
        functools.partial(complete, features=width * kv_count),
        jax.ShapeDtypeStruct((rows + TAIL + 2 * (share + TAIL), HD), BF16),
        [SMEM] + [VMEM] * 3,
        2 * kv_count * rows * HD,
        2 * kv_count * rows * HD,
        name="complete",
    )(where, parts, cosines, sines)
    there = lax.ppermute(here, "tp", swap)
    query_here = jnp.where(
        lax.rem(kv_index, 2) == 0, here[: rows + TAIL], there[: rows + TAIL]
    )
    queries = lax.all_gather(query_here, both, axis=0, axis_index_groups=lines)

    own, above, below = call(
        functools.partial(attend, group=4),
        (
            jax.ShapeDtypeStruct((near, HD + TAIL, rows), BF16),
            jax.ShapeDtypeStruct((near // 2, HD + TAIL, rows), BF16),
            jax.ShapeDtypeStruct((near - near // 2, HD + TAIL, rows), BF16),
        ),
        [SMEM] * 5 + [VMEM] * 5 + [HBM],
        4 * tokens * heads * block * HD,
        kv_cache.size,
        [
            pltpu.VMEM((share + TAIL, HD), F32),
            pltpu.VMEM((HD, HD), F32),
            pltpu.VMEM((16, HD), F32),
            pltpu.VMEM((members, HD, block), BF16),
            pltpu.VMEM((members, block, HD), F32),
            pltpu.VMEM((members + steps, block, 2 * HD), BF16),
            pltpu.VMEM((kv_count, HD + TAIL, rows), BF16),
            pltpu.SemaphoreType.DMA((members + steps,)),
        ],
        "attend",
        limit=52 << 20,
    )(
        where,
        starts,
        rollout_ids,
        resume_offsets,
        step_lengths,
        queries,
        here,
        there,
        cosines,
        sines,
        kv_cache,
    )

    def crossed(value, step):
        return lax.ppermute(
            value,
            both,
            [
                (t * kv_count + z, (t ^ 1) * kv_count + (z + step) % kv_count)
                for t in range(tp_count)
                for z in range(kv_count)
            ],
        )

    mixed = call(
        unite,
        jax.ShapeDtypeStruct((near, HD + TAIL, rows), BF16),
        [VMEM] * 3,
        near * HD * rows,
        8 * near * HD * rows,
        name="unite",
    )(own, crossed(above, 1), crossed(below, -1))
    mixed_mine = lax.dynamic_index_in_dim(mixed, kv_index // 2, 0, keepdims=False)
    mixed = lax.all_to_all(mixed, both, 0, 0, tiled=True, axis_index_groups=strides)
    mix_here = call(
        combine,
        jax.ShapeDtypeStruct((rows + TAIL, HD), BF16),
        [SMEM] + [VMEM] * 2,
        2 * kv_count * rows * HD,
        2 * kv_count * rows * HD,
        name="combine",
    )(where, mixed, mixed_mine)
    mix = lax.all_gather(mix_here, both, axis=0, axis_index_groups=lines)
    shares = call(
        functools.partial(deliver, steps=steps),
        jax.ShapeDtypeStruct((tp_count, w_output.shape[1] // HD * taken + TAIL, HD), BF16),
        [SMEM] + [VMEM] * 3,
        2 * tokens * w_output.size,
        4 * w_output.size,
        [pltpu.VMEM((16, w_output.shape[0]), F32)],
        "deliver",
    )(where, mix, w_output, w_output_there)
    shares_mine = lax.dynamic_index_in_dim(shares, tp_index, 0, keepdims=False)
    shares = lax.all_to_all(shares, "tp", 0, 0, tiled=True)
    return call(
        settle,
        (
            jax.ShapeDtypeStruct((taken, w_output.shape[1]), BF16),
            jax.ShapeDtypeStruct((steps, w_output.shape[1]), BF16),
        ),
        [SMEM] + [VMEM] * 2,
        2 * tokens * w_output.shape[1],
        2 * tokens * w_output.shape[1],
        name="settle",
    )(where, shares, shares_mine)


def solution(mesh):
    in_specs = (
        P("groups", "kv"),
        P("groups", "kv"),
        P("kv"),
        P("kv", "tp"),
        P("kv", "tp"),
        P("kv", "tp"),
        P("tp", "kv"),
        P("groups", "kv", "tp"),
        P("groups"),
        P("groups"),
        P("groups"),
        P("groups"),
    )
    out_specs = (P(("groups", "tp"), "kv"), P("groups", "kv"))
    return jax.shard_map(
        on_device, mesh=mesh, in_specs=in_specs, out_specs=out_specs, check_vma=False
    )
```

```python
import functools
import math

import jax
import jax.numpy as jnp
from jax import lax
from jax.experimental import pallas as pl
from jax.experimental.pallas import tpu as pltpu
from jax.sharding import PartitionSpec as P

HD = 128
SEQS = 2
EPSILON = 1e-05
THETA = 500000.0
NEGATIVE = -1e30
TAIL = 8
F32 = jnp.float32
BF16 = jnp.bfloat16
VMEM = pltpu.VMEM
SMEM = pltpu.SMEM
HBM = pltpu.HBM


def call(body, outs, spaces, flops, traffic, scratch=(), name=None, limit=20 << 20):
    return pl.pallas_call(
        body,
        out_shape=outs,
        in_specs=[pl.BlockSpec(memory_space=s) for s in spaces],
        out_specs=jax.tree.map(lambda _: pl.BlockSpec(memory_space=VMEM), outs),
        scratch_shapes=list(scratch),
        compiler_params=pltpu.CompilerParams(vmem_limit_bytes=limit),
        cost_estimate=pl.CostEstimate(flops=flops, bytes_accessed=traffic, transcendentals=0),
        name=name,
    )


def two_terms(value):
    high = value.astype(BF16).astype(F32)
    return high, value - high


def three_terms(value):
    high, rest = two_terms(value)
    mid, low = two_terms(rest)
    return high, mid, low


def stacked_rows(rows):
    place = lax.broadcasted_iota(jnp.int32, (TAIL, HD), 0)
    block = jnp.zeros((TAIL, HD), F32)
    for k, row in enumerate(rows):
        block = jnp.where(place == k, jnp.broadcast_to(row, (TAIL, HD)), block)
    return block


def turned(values, cosines, sines):
    half = HD // 2
    swapped = jnp.concatenate([values[:, half:], values[:, :half]], axis=1)
    return values * cosines + swapped * sines


def partial_products(rows_ref, step_rows, scale, w_query, w_pair, flip, put):
    near, share = put.near, rows_ref.shape[0] // put.near
    heads = w_query.shape[1] // HD
    steps, width = step_rows.shape
    dims = (((1,), (1,)), ((), ()))
    wide = rows_ref[...].astype(F32)
    normed = (wide * scale).astype(BF16)
    high, low = two_terms(wide * wide)
    ones = jnp.ones((TAIL, width), BF16)
    sums = lax.dot_general(ones, high.astype(BF16), dims, preferred_element_type=F32)
    sums = sums + lax.dot_general(ones, low.astype(BF16), dims, preferred_element_type=F32)
    sums = sums[0:1, :]
    step_wide = jnp.concatenate([step_rows, jnp.zeros((TAIL - steps, width), F32)], axis=0)
    step_normed = (step_wide * scale).astype(BF16)
    step_sums = jnp.sum(step_wide * step_wide, axis=1, keepdims=True)
    step_pieces = []
    for c in range(0, heads, 2):
        weight = w_query[:, c * HD : (c + 2) * HD]
        part = jnp.dot(normed, weight, preferred_element_type=F32)
        put(c * share, part[:, :HD].reshape(near, share, HD))
        put((c + 1) * share, part[:, HD:].reshape(near, share, HD))
        small = jnp.dot(step_normed, weight, preferred_element_type=F32)
        step_pieces += [small[:, :HD], small[:, HD:]]
    pair = w_pair()
    part = lax.dot_general(normed, pair, dims, preferred_element_type=F32)
    put(heads * share, part.reshape(near, share, HD))
    step_pieces.append(lax.dot_general(step_normed, pair, dims, preferred_element_type=F32))

    def step_part(d):
        s, c = divmod(d, heads + 1)
        if s >= steps:
            return jnp.zeros((1, HD), F32), jnp.zeros((1, HD), F32)
        return step_pieces[c][s : s + 1, :], jnp.broadcast_to(step_sums[s : s + 1, :], (1, HD))

    tails = []
    for k in range(near):
        lane = k * share // HD * HD
        piece, total = (
            jnp.where(flip, b, a) for a, b in zip(step_part(2 * k), step_part(2 * k + 1))
        )
        tails.append(
            stacked_rows([piece, *two_terms(sums[:, lane : lane + HD]), *two_terms(total)])[None]
        )
    put((heads + 1) * share, jnp.concatenate(tails, axis=0))


class Split:
    def __init__(self, *outs):
        self.outs = outs
        self.near = sum(out.shape[0] for out in outs)

    def __call__(self, start, value):
        at = 0
        for out in self.outs:
            end = at + out.shape[0]
            out[:, start : start + value.shape[1], :] = value[at:end].astype(out.dtype)
            at = end


def project(prompt_in, step_in, gain_in, query_in, key_in, value_in, *refs, home):
    *outs, prompt, step_rows, gain, w_query, w_pair, sems = refs
    put = Split(*outs)
    share = prompt.shape[0] // put.near
    half = key_in.shape[0]
    parity = lax.rem(lax.axis_index("kv") + (0 if home else 1), 2)
    pairs = [
        (
            prompt_in.at[
                pl.ds(pl.multiple_of((2 * k + parity) * share, share), share), :
            ],
            prompt.at[k * share : (k + 1) * share, :],
        )
        for k in range(put.near)
    ]
    pairs += [
        (gain_in, gain),
        (step_in, step_rows),
        (query_in, w_query),
        (key_in, w_pair.at[0:half, :]),
        (value_in, w_pair.at[half : 2 * half, :]),
    ]
    moves = [
        pltpu.make_async_copy(source, target, sems.at[k])
        for k, (source, target) in enumerate(pairs)
    ]
    for move in moves:
        move.start()
    for move in moves:
        move.wait()
    scale = gain[...].astype(F32).reshape(1, gain.shape[0])
    partial_products(
        prompt, step_rows[...].astype(F32), scale, w_query, lambda: w_pair[...], parity == 1, put
    )


def merge(own, under, over, out):
    near, size, _ = own.shape
    start = size - TAIL
    for k in range(near):
        other = under[k] if k < under.shape[0] else over[k - under.shape[0]]
        both = own[k] + other.astype(F32)
        out[k, 0:start, :] = both[:start, :].astype(BF16)
        tail = both[start:, :]
        out[k, start:, :] = stacked_rows(
            [
                tail[0:1, :],
                *two_terms(tail[1:2, :] + tail[2:3, :]),
                *two_terms(tail[3:4, :] + tail[4:5, :]),
            ]
        ).astype(BF16)


def complete(where, tiles, cosines, sines, out, *, features):
    count = tiles.shape[0]
    share = cosines.shape[0] - TAIL
    heads = (out.shape[0] - 3 * TAIL) // share - 2

    def total(start, size):
        return jnp.sum(tiles[:, start : start + size, :].astype(F32), axis=0)

    tail = total((heads + 1) * share, TAIL)
    row_scale = lax.rsqrt((tail[1:2, :] + tail[2:3, :]) / features + EPSILON)
    offset = lax.rem(where[0] // 2 * share, HD)
    place = lax.broadcasted_iota(jnp.int32, (share, HD), 0) + offset
    lane = lax.broadcasted_iota(jnp.int32, (share, HD), 1)
    scale = jnp.sum(
        jnp.where(place == lane, jnp.broadcast_to(row_scale, (share, HD)), 0.0),
        axis=1,
        keepdims=True,
    )
    step_scale = lax.rsqrt((tail[3:4, :] + tail[4:5, :]) / features + EPSILON)
    first = lax.broadcasted_iota(jnp.int32, (TAIL, HD), 0) == 0
    step_value = jnp.where(first, jnp.broadcast_to(tail[0:1, :] * step_scale, (TAIL, HD)), 0.0)
    cosine, sine = cosines[0:share, :], sines[0:share, :]
    for c in range(heads):
        value = total(c * share, share) * scale
        out[c * share : (c + 1) * share, :] = turned(value, cosine, sine).astype(BF16)
    out[heads * share : heads * share + TAIL, :] = turned(
        step_value, cosines[share:, :], sines[share:, :]
    ).astype(BF16)
    at = heads * share + TAIL
    for high_low in zip(two_terms(total(heads * share, share) * scale), two_terms(step_value)):
        out[at : at + share, :] = high_low[0].astype(BF16)
        out[at + share : at + share + TAIL, :] = high_low[1].astype(BF16)
        at += share + TAIL


def attend(
    where,
    starts,
    slots,
    offsets,
    lengths,
    queries,
    own_part,
    other_part,
    cosines,
    sines,
    cache_in,
    own_out,
    above_out,
    below_out,
    own_keys,
    own_values,
    step_query,
    values,
    bias,
    cache,
    out,
    sems,
    *,
    group,
):
    count = queries.shape[0]
    share = cosines.shape[0] - TAIL
    heads = (queries.shape[1] - TAIL) // share
    rows = heads * share
    members = slots.shape[0]
    steps = lengths.shape[0]
    block = cache.shape[1]
    half = HD // 2
    moves = [
        pltpu.make_async_copy(
            cache_in.at[SEQS + slots[k] if k < members else k - members],
            cache.at[k],
            sems.at[k],
        )
        for k in range(members + steps)
    ]
    for move in moves:
        move.start()
    mine = where[0]
    parity = lax.rem(mine, 2)
    first = where[1] == 0
    base2 = math.log2(math.e)
    root = base2 / math.sqrt(HD)

    def pair_of(part):
        at = rows + TAIL
        high = part[at : at + share + TAIL, :].astype(F32)
        return high + part[at + share + TAIL : at + 2 * (share + TAIL), :].astype(F32)

    own_pair, other_pair = pair_of(own_part), pair_of(other_part)
    low_half = jnp.where(first, own_pair, other_pair)
    high_half = jnp.where(first, other_pair, own_pair)
    raw_keys = jnp.concatenate([low_half[:, :half], high_half[:, :half]], axis=1)
    raw_values = jnp.concatenate([low_half[:, half:], high_half[:, half:]], axis=1)
    own_keys[...] = turned(raw_keys, cosines[...], sines[...])
    own_values[...] = jnp.zeros_like(own_values)
    own_values[0 : share + TAIL, :] = raw_values
    keys_here = own_keys[0:share, :].astype(BF16)
    values_here = jnp.transpose(own_values[...])[:, 0:share].astype(BF16)
    dims = (((1,), (1,)), ((), ()))
    key_place = lax.broadcasted_iota(jnp.int32, (1, block), 1) + mine * block
    tile = group * rows
    lane = lax.broadcasted_iota(jnp.int32, (share, tile), 1)
    token_in_tile = lane // rows * share + lax.rem(lane, share)
    key_token = mine * share + lax.broadcasted_iota(jnp.int32, (share, tile), 0)

    key_column = lax.broadcasted_iota(jnp.int32, (block, HD), 0) + mine * block
    for r in range(members):
        moves[r].wait()
        for k in range(0, block, HD):
            values[r, :, k : k + HD] = jnp.transpose(
                cache[r, k : k + HD, HD:].astype(F32)
            ).astype(BF16)
        bias[r] = jnp.where(key_column < offsets[r], 0.0, NEGATIVE)

    step_rows = {}
    for s in range(steps):
        moves[members + s].wait()
        step_query[...] = jnp.zeros_like(step_query)
        for h in range(heads):
            step_query[h : h + 1, :] = queries[s * (heads + 1) + h, rows : rows + TAIL, :].astype(
                F32
            )[0:1, :]
        query = step_query[...]
        scores = lax.dot_general(
            query.astype(BF16), cache[members + s, :, 0:HD], dims, preferred_element_type=F32
        ) * root + jnp.where(key_place < lengths[s], 0.0, NEGATIVE)
        own_key = own_keys[share : share + 1, :].astype(BF16).astype(F32)
        own_value = own_values[share : share + 1, :].astype(BF16).astype(F32)
        own = jnp.sum(query * own_key, axis=1, keepdims=True) * root
        own = jnp.where(mine == s * (heads + 1) + heads, own, NEGATIVE)
        top = jnp.maximum(jnp.max(scores, axis=1, keepdims=True), own)
        weights = jnp.exp2(scores - top)
        own_weight = jnp.exp2(own - top)
        denominator = jnp.sum(weights, axis=1, keepdims=True) + own_weight
        mixed = jnp.dot(weights.astype(BF16), cache[members + s, :, HD:], preferred_element_type=F32)
        mixed = mixed + own_weight.astype(BF16).astype(F32) * own_value
        mixed = mixed / denominator
        level = top + jnp.log(denominator) * base2
        for h in range(heads):
            step_rows[s * heads + h] = [mixed[h : h + 1, :]] + [
                jnp.broadcast_to(t, (1, HD)) for t in three_terms(level[h : h + 1, :])
            ]

    for t in range(count // group):
        begin = t * group * share
        token = token_in_tile + begin
        query = queries[t * group : (t + 1) * group, 0:rows, :].reshape(tile, HD)

        for r in range(members):
            since = starts[r]
            until = starts[r + 1]

            @pl.when((since < begin + group * share) & (until > begin))
            def _():
                scored = lax.dot_general(keys_here, query, dims, preferred_element_type=F32)
                own = jnp.where((key_token >= since) & (key_token <= token), scored, NEGATIVE)
                limit = jnp.concatenate([bias[r]] * (tile // HD), axis=1)
                scores = (
                    lax.dot_general(
                        cache[r, :, 0:HD], query, dims, preferred_element_type=F32
                    )
                    + limit
                )
                top = jnp.maximum(
                    jnp.max(scores, axis=0, keepdims=True), jnp.max(own, axis=0, keepdims=True)
                )
                weights = jnp.exp2((scores - top) * root)
                own_weights = jnp.exp2((own - top) * root)
                denominator = jnp.sum(weights, axis=0, keepdims=True) + jnp.sum(
                    own_weights, axis=0, keepdims=True
                )
                mixed = jnp.dot(values[r], weights.astype(BF16), preferred_element_type=F32)
                mixed = mixed + jnp.dot(
                    values_here, own_weights.astype(BF16), preferred_element_type=F32
                )
                mixed = mixed / denominator
                level = top * root + jnp.log(denominator) * base2
                for g in range(group):
                    d = t * group + g
                    at = d // 2 + jnp.where(parity == d % 2, 0, count // 2)
                    piece = mixed[:, g * rows : (g + 1) * rows]
                    flat = level[:, g * rows : (g + 1) * rows]
                    tail = stacked_rows(list(three_terms(flat)) + step_rows.get(d, []))

                    @pl.when(since <= begin + g * share)
                    def _():
                        out[at, 0:HD, :] = piece.astype(BF16)
                        out[at, HD : HD + TAIL, :] = tail.astype(BF16)

                    @pl.when(since > begin + g * share)
                    def _():
                        late = token[:, g * rows : (g + 1) * rows][0:1, :] >= since
                        before = out[at, 0:HD, :].astype(F32)
                        out[at, 0:HD, :] = jnp.where(late, piece, before).astype(BF16)
                        earlier = out[at, HD : HD + TAIL, :].astype(F32)
                        out[at, HD : HD + TAIL, :] = jnp.where(late, tail, earlier).astype(BF16)

    near, part_count = own_out.shape[0], above_out.shape[0]
    own_out[...] = out[0:near]
    above_out[...] = out[near : near + part_count]
    below_out[...] = out[near + part_count :]


def unite(own, under, over, out):
    for k in range(own.shape[0]):
        other = under[k] if k < under.shape[0] else over[k - under.shape[0]]
        one, two = own[k].astype(F32), other.astype(F32)
        tails = one[HD:, :], two[HD:, :]

        def shares(at):
            first, second = (t[at : at + 1] + t[at + 1 : at + 2] + t[at + 2 : at + 3] for t in tails)
            top = jnp.maximum(first, second)
            first, second = jnp.exp2(first - top), jnp.exp2(second - top)
            total = first + second
            return first / total, second / total, top + jnp.log(total) * math.log2(math.e)

        left, right, level = shares(0)
        out[k, 0:HD, :] = (one[:HD, :] * left + two[:HD, :] * right).astype(BF16)
        left, right, step_level = shares(4)
        step = tails[0][3:4] * left + tails[1][3:4] * right
        out[k, HD:, :] = stacked_rows(
            [*three_terms(level), step, *three_terms(step_level)]
        ).astype(BF16)


def combine(tiles, out):
    rows = tiles.shape[2]
    tail = tiles[:, HD : HD + TAIL, :].astype(F32)

    def shares(at):
        level = tail[:, at, :] + tail[:, at + 1, :] + tail[:, at + 2, :]
        weight = jnp.exp2(level - jnp.max(level, axis=0, keepdims=True))
        return weight / jnp.sum(weight, axis=0, keepdims=True)

    weight = shares(0)
    mixed = jnp.zeros((HD, rows), F32)
    for k in range(tiles.shape[0]):
        mixed = mixed + weight[k : k + 1, :] * tiles[k, 0:HD, :].astype(F32)
    out[0:rows, :] = jnp.transpose(mixed).astype(BF16)
    step = jnp.sum(shares(4) * tail[:, 3, :], axis=0, keepdims=True)
    out[rows : rows + TAIL, :] = jnp.broadcast_to(step, (TAIL, HD)).astype(BF16)


def deliver(where, mix, w_here, w_there, own_out, other_out, step_pad, out, *, steps):
    count = mix.shape[0]
    heads = w_here.shape[0] // HD
    share = (mix.shape[1] - TAIL) // heads
    takers = out.shape[0]
    wide = w_here.shape[1] // HD
    taken = count * share // takers
    step_pad[...] = jnp.zeros_like(step_pad)
    for s in range(steps):
        for h in range(heads):
            step_pad[s : s + 1, h * HD : (h + 1) * HD] = mix[
                s * heads + h, heads * share : heads * share + TAIL, :
            ].astype(F32)[0:1, :]

    def project_with(w_output):
        block = jnp.concatenate(
            [
                mix[:, h * share : (h + 1) * share, :].reshape(count * share, HD)
                for h in range(heads)
            ],
            axis=1,
        )
        small = jnp.dot(step_pad[...].astype(BF16), w_output[...], preferred_element_type=F32)
        tail = stacked_rows(
            [small[s : s + 1, c * HD : (c + 1) * HD] for s in range(steps) for c in range(wide)]
        ).astype(BF16)
        for c in range(0, wide, 2):
            part = jnp.dot(
                block, w_output[:, c * HD : (c + 2) * HD], preferred_element_type=F32
            ).astype(BF16)
            for k in range(2):
                out[:, (c + k) * taken : (c + k + 1) * taken, :] = part[
                    :, k * HD : (k + 1) * HD
                ].reshape(takers, taken, HD)
        for d in range(takers):
            out[d, wide * taken : wide * taken + TAIL, :] = tail

    pl.when(lax.rem(where[0], 2) == 0)(lambda: project_with(w_here))
    pl.when(lax.rem(where[0], 2) == 1)(lambda: project_with(w_there))
    for k in range(takers // 2):
        own_out[k] = out[2 * k + where[1]]
        other_out[k] = out[2 * k + 1 - where[1]]


def add_up(own, other, out):
    out[...] = (own[...].astype(F32) + other[...].astype(F32)).astype(BF16)


def settle(tiles, prompt_out, step_out):
    taken, width = prompt_out.shape
    wide = width // HD
    for c in range(wide):
        prompt_out[:, c * HD : (c + 1) * HD] = jnp.sum(
            tiles[:, c * taken : (c + 1) * taken, :].astype(F32), axis=0
        ).astype(BF16)
    tail = jnp.sum(tiles[:, wide * taken : wide * taken + TAIL, :].astype(F32), axis=0)
    for s in range(step_out.shape[0]):
        for c in range(wide):
            step_out[s : s + 1, c * HD : (c + 1) * HD] = tail[
                s * wide + c : s * wide + c + 1, :
            ].astype(BF16)


def on_device(
    prompt_rows,
    step_rows,
    norm_gain,
    w_query,
    w_key,
    w_value,
    w_output,
    kv_cache,
    step_lengths,
    rollout_ids,
    resume_offsets,
    stretch_rollout,
):
    kv_index = lax.axis_index("kv")
    kv_count = lax.axis_size("kv")
    tp_index = lax.axis_index("tp")
    tp_count = lax.axis_size("tp")
    tokens, width = prompt_rows.shape
    steps = step_rows.shape[0]
    heads = w_query.shape[1] // HD
    share = tokens // kv_count
    taken = tokens // tp_count
    rows = heads * share
    members = resume_offsets.shape[0]
    where = jnp.stack([kv_index, lax.rem(tp_index, 2)]).astype(jnp.int32)

    swap = [(k, k ^ 1) for k in range(tp_count)]
    lines = [
        [(pair * 2 + (core ^ (z & 1))) * kv_count + z for z in range(kv_count)]
        for pair in range(tp_count // 2)
        for core in range(2)
    ]

    both = ("tp", "kv")
    near = kv_count // 2
    size = rows + share + TAIL

    def shifted(value, step):
        return lax.ppermute(
            value, "kv", [(z, (z + step) % kv_count) for z in range(kv_count)]
        )

    def projected(outs, operands, home):
        return call(
            functools.partial(project, home=home),
            outs,
            [HBM] * 6,
            tokens * width * (w_query.shape[1] + HD),
            4 * tokens * width,
            [
                pltpu.VMEM((tokens // 2, width), BF16),
                pltpu.VMEM((steps, width), BF16),
                pltpu.VMEM((width,), BF16),
                pltpu.VMEM(w_query.shape, BF16),
                pltpu.VMEM((HD, width), BF16),
                pltpu.SemaphoreType.DMA((5 + near,)),
            ],
            "project_home" if home else "project_away",
            limit=60 << 20,
        )(*operands)

    operands = (prompt_rows, step_rows, norm_gain, w_query, w_key.T, w_value.T)
    above, below = projected(
        (
            jax.ShapeDtypeStruct((near // 2, size, HD), BF16),
            jax.ShapeDtypeStruct((near - near // 2, size, HD), BF16),
        ),
        operands,
        False,
    )
    above, below, operands = lax.optimization_barrier((above, below, operands))
    own = projected(jax.ShapeDtypeStruct((near, size, HD), F32), operands, True)
    parts = call(
        merge,
        jax.ShapeDtypeStruct((near, size, HD), BF16),
        [VMEM] * 3,
        near * size * HD,
        8 * near * size * HD,
        name="merge",
    )(own, shifted(above, 1), shifted(below, -1))
    parts, w_output = lax.optimization_barrier((parts, w_output))
    w_output_there = lax.ppermute(w_output, "tp", swap)
    strides = [
        [t * kv_count + z for z in range(parity, kv_count, 2)]
        for t in range(tp_count)
        for parity in range(2)
    ]
    parts = lax.all_to_all(parts, both, 0, 0, tiled=True, axis_index_groups=strides)

    member_index = jnp.arange(members + 1, dtype=jnp.int32)
    starts = jnp.sum(
        (stretch_rollout[:, None] < member_index[None, :]).astype(jnp.int32), axis=0
    )
    tokens_here = kv_index * share + jnp.arange(share, dtype=jnp.int32)
    rollout_here = jnp.sum(
        (tokens_here[:, None] >= starts[None, 1:members]).astype(jnp.int32), axis=1
    )
    onehot = (rollout_here[:, None] == member_index[None, :members]).astype(jnp.int32)
    positions = jnp.sum(onehot * (resume_offsets - starts[:members])[None, :], axis=1) + tokens_here
    step_place = jnp.minimum(kv_index // (heads + 1), steps - 1)
    step_position = lax.dynamic_slice_in_dim(step_lengths, step_place, 1, 0)
    positions = jnp.concatenate([positions, jnp.broadcast_to(step_position, (TAIL,))])
    half = HD // 2
    inverse = jnp.exp(jnp.arange(half, dtype=F32) * (-2.0 * math.log(THETA) / HD))
    angles = positions.astype(F32)[:, None] * inverse[None, :]
    cosine, sine = jnp.cos(angles), jnp.sin(angles)
    cosines = jnp.concatenate([cosine, cosine], axis=1)
    sines = jnp.concatenate([-sine, sine], axis=1)

    block = kv_cache.shape[1]
    parts, w_output_there = lax.optimization_barrier((parts, w_output_there))
    here = call(
        functools.partial(complete, features=width * kv_count),
        jax.ShapeDtypeStruct((rows + TAIL + 2 * (share + TAIL), HD), BF16),
        [SMEM] + [VMEM] * 3,
        2 * kv_count * rows * HD,
        2 * kv_count * rows * HD,
        name="complete",
    )(where, parts, cosines, sines)
    there = lax.ppermute(here, "tp", swap)
    query_here = jnp.where(
        lax.rem(kv_index, 2) == 0, here[: rows + TAIL], there[: rows + TAIL]
    )
    queries = lax.all_gather(query_here, both, axis=0, axis_index_groups=lines)

    own, above, below = call(
        functools.partial(attend, group=4),
        (
            jax.ShapeDtypeStruct((near, HD + TAIL, rows), BF16),
            jax.ShapeDtypeStruct((near // 2, HD + TAIL, rows), BF16),
            jax.ShapeDtypeStruct((near - near // 2, HD + TAIL, rows), BF16),
        ),
        [SMEM] * 5 + [VMEM] * 5 + [HBM],
        4 * tokens * heads * block * HD,
        kv_cache.size,
        [
            pltpu.VMEM((share + TAIL, HD), F32),
            pltpu.VMEM((HD, HD), F32),
            pltpu.VMEM((16, HD), F32),
            pltpu.VMEM((members, HD, block), BF16),
            pltpu.VMEM((members, block, HD), F32),
            pltpu.VMEM((members + steps, block, 2 * HD), BF16),
            pltpu.VMEM((kv_count, HD + TAIL, rows), BF16),
            pltpu.SemaphoreType.DMA((members + steps,)),
        ],
        "attend",
        limit=52 << 20,
    )(
        where,
        starts,
        rollout_ids,
        resume_offsets,
        step_lengths,
        queries,
        here,
        there,
        cosines,
        sines,
        kv_cache,
    )

    def crossed(value, step):
        return lax.ppermute(
            value,
            both,
            [
                (t * kv_count + z, (t ^ 1) * kv_count + (z + step) % kv_count)
                for t in range(tp_count)
                for z in range(kv_count)
            ],
        )

    mixed = call(
        unite,
        jax.ShapeDtypeStruct((near, HD + TAIL, rows), BF16),
        [VMEM] * 3,
        near * HD * rows,
        8 * near * HD * rows,
        name="unite",
    )(own, crossed(above, 1), crossed(below, -1))
    mixed = lax.all_to_all(mixed, both, 0, 0, tiled=True, axis_index_groups=strides)
    mix_here = call(
        combine,
        jax.ShapeDtypeStruct((rows + TAIL, HD), BF16),
        [VMEM],
        2 * kv_count * rows * HD,
        2 * kv_count * rows * HD,
        name="combine",
    )(mixed)
    mix = lax.all_gather(mix_here, both, axis=0, axis_index_groups=lines)
    slot = (w_output.shape[1] // HD * taken + TAIL, HD)
    half_slots = jax.ShapeDtypeStruct((tp_count // 2, *slot), BF16)
    own, other = call(
        functools.partial(deliver, steps=steps),
        (half_slots, half_slots),
        [SMEM] + [VMEM] * 3,
        2 * tokens * w_output.size,
        4 * w_output.size,
        [
            pltpu.VMEM((16, w_output.shape[0]), F32),
            pltpu.VMEM((tp_count, *slot), BF16),
        ],
        "deliver",
    )(where, mix, w_output, w_output_there)
    shares = call(
        add_up,
        half_slots,
        [VMEM] * 2,
        tokens * w_output.shape[1],
        3 * tokens * w_output.shape[1],
        name="add_up",
    )(own, lax.ppermute(other, "tp", swap))
    columns = [
        [t * kv_count + z for t in range(core, tp_count, 2)]
        for core in range(2)
        for z in range(kv_count)
    ]
    shares = lax.all_to_all(shares, both, 0, 0, tiled=True, axis_index_groups=columns)
    return call(
        settle,
        (
            jax.ShapeDtypeStruct((taken, w_output.shape[1]), BF16),
            jax.ShapeDtypeStruct((steps, w_output.shape[1]), BF16),
        ),
        [VMEM],
        2 * tokens * w_output.shape[1],
        2 * tokens * w_output.shape[1],
        name="settle",
    )(shares)


def solution(mesh):
    in_specs = (
        P("groups", "kv"),
        P("groups", "kv"),
        P("kv"),
        P("kv", "tp"),
        P("kv", "tp"),
        P("kv", "tp"),
        P("tp", "kv"),
        P("groups", "kv", "tp"),
        P("groups"),
        P("groups"),
        P("groups"),
        P("groups"),
    )
    out_specs = (P(("groups", "tp"), "kv"), P("groups", "kv"))
    return jax.shard_map(
        on_device, mesh=mesh, in_specs=in_specs, out_specs=out_specs, check_vma=False
    )
```
